256 devices in a mesh: grp: 8 (over z), pen: 32 (over y, x, core).
Axes of the slice: x: 4, y: 4, z: 8, core: 2. Of those that a mesh axis runs over, the one named last changes fastest.
Arguments:
- cell_offsets: int32 [2, 1048576], P(None, ('grp', 'pen')), may hold values from 0 to 1
- cell_z: int32 [1048576], P(('grp', 'pen')), may hold values from 0 to 255
- frac: float32 [3, 1048576], P(None, ('grp', 'pen')), may hold values from 0 to 1
- charges: float32 [1048576], P(('grp', 'pen')), may hold values from -4 to 4
- tile_counts: int32 [16384], P(('grp', 'pen')), may hold values from 16 to 64, as said below
Outputs:
- forces: float32 [3, 1048576], P(None, ('grp', 'pen'))
- energy: float32 [], replicated
The draws below stay inside these ranges and needn't reach their ends.
Inputs may be any that keep to these rules, and one draw needn't show every extreme that they name: `tile_counts`: live slots of each tile; some tile holds 64.
All inputs are finite; a program needn't handle non-finite values.
Results may differ from the reference program's by a relative error of at most 0.0003.
Values sent between devices are 32-bit elements; how exact they have to be, the bound alone decides.
No kernel may reach another device: no remote copies, remote signals or barrier semaphores. Data moves between devices by JAX's collectives and lax.ppermute only.
A program may use at most 128 MiB of HBM per device.

```python
import math
import jax
import jax.numpy as jnp
from jax import lax

KX = 256
KY = 256
KZ = 256
SLOTS = 64
TILES = 16384
ATOMS = 1048576
N_GRP = 8
N_PEN = 32


def draw_tile_counts(key, part):
    counts = jax.random.randint(key, (TILES,), max(1, SLOTS // 4), SLOTS + 1)
    filled = jax.random.randint(jax.random.fold_in(key, 7), (), 0, TILES)
    return counts.at[filled].set(SLOTS).astype(jnp.int32)


def place_ends(drawn, key, low, top_value):
    dims = drawn.shape
    spot = [jax.random.randint(jax.random.fold_in(key, axis), (), 0, dims[axis]) for axis in range(len(dims))]
    drawn = drawn.at[tuple(spot)].set(low)
    longest = dims.index(max(dims))
    spot[longest] = (spot[longest] + 1) % dims[longest]
    return drawn.at[tuple(spot)].set(top_value)


def steps_of(own_key, shape, cuts, least, high):
    gain, own = 1.0, jax.random.fold_in(own_key, 6)
    for axis_at, shards_of in cuts:
        steps = jnp.exp(jax.random.uniform(jax.random.fold_in(own, axis_at), (shards_of,), jnp.float32, least / len(cuts), high / len(cuts)))
        gain = gain * jnp.repeat(steps, shape[axis_at] // shards_of).reshape([-1 if axis == axis_at else 1 for axis in range(len(shape))])
    return gain


def scatter_about(stream_key, shape, width, limit, shards=(), kind=jnp.bfloat16):
    array = jax.random.normal(stream_key, shape, jnp.float32) * width
    if len(shards) > 0:
        array = steps_of(stream_key, shape, shards, -0.22, 0.18) * array
    return jnp.clip(array, min=-limit, max=limit).astype(kind)


def setup_inputs(seed: int = 0) -> dict:
    arg_keys = jax.random.split(jax.random.key(seed), 6)
    return {
        "cell_offsets": place_ends(jax.random.randint(arg_keys[0], (2, ATOMS), 0, 2), jax.random.fold_in(arg_keys[0], 1), 0, 1).astype(jnp.int32),
        "cell_z": place_ends(jax.random.randint(arg_keys[1], (ATOMS,), 0, KZ), jax.random.fold_in(arg_keys[1], 1), 0, KZ - 1).astype(jnp.int32),
        "frac": jnp.clip(1.0 * jax.random.uniform(arg_keys[2], (3, ATOMS), jnp.float32) ** steps_of(arg_keys[2], (3, ATOMS), ((1, 256),), -0.2, 0.2), 0.0, 1.0),
        "charges": scatter_about(arg_keys[3], (ATOMS,), 1.0, 4.0, ((0, 256),), jnp.float32),
        "tile_counts": draw_tile_counts(jax.random.fold_in(arg_keys[5], 71), 0),
    }


ewald_split = 0.6


def spline_rows(fracs):
    values = [jnp.ones_like(fracs)]
    fifth = values
    for order in range(2, 7):
        nxt = []
        for j in range(order):
            term = jnp.zeros_like(fracs)
            if j >= 1:
                term = term + values[j - 1] * (fracs + order - 1 - j)
            if j <= order - 2:
                term = term + values[j] * (1.0 - fracs + j)
            nxt.append(term / (order - 1))
        if order == 5:
            fifth = nxt
        values = nxt
    slopes = []
    for j in range(6):
        term = jnp.zeros_like(fracs)
        if j >= 1:
            term = term + fifth[j - 1]
        if j <= 4:
            term = term - fifth[j]
        slopes.append(term)
    return values, slopes


def tile_weights(offsets, zcell, fracs, charge, counts, size_z):
    slots = charge.shape[-1]
    live = (jnp.arange(slots, dtype=jnp.int32) < counts[..., None]).astype(jnp.float32)
    live_q = charge * live
    theta_x, slope_x = spline_rows(fracs[0])
    theta_y, slope_y = spline_rows(fracs[1])
    theta_z, slope_z = spline_rows(fracs[2])
    footing = jnp.arange(8, dtype=jnp.int32)[:, None]
    cells = jnp.arange(size_z, dtype=jnp.int32)
    weight_x = 0.0
    grade_x = 0.0
    weight_y = 0.0
    grade_y = 0.0
    weight_z = 0.0
    grade_z = 0.0
    for j in range(6):
        hit_x = (footing == offsets[0][..., None, :] + j).astype(jnp.float32)
        hit_y = (footing == offsets[1][..., None, :] + j).astype(jnp.float32)
        hit_z = (cells == (zcell[..., :, None] + j) % size_z).astype(jnp.float32)
        weight_x = weight_x + theta_x[j][..., None, :] * hit_x
        grade_x = grade_x + slope_x[j][..., None, :] * hit_x
        weight_y = weight_y + theta_y[j][..., None, :] * hit_y
        grade_y = grade_y + slope_y[j][..., None, :] * hit_y
        weight_z = weight_z + theta_z[j][..., :, None] * hit_z
        grade_z = grade_z + slope_z[j][..., :, None] * hit_z
    return weight_x, grade_x, weight_y, grade_y, weight_z, grade_z, live_q


def modulus(index, length):
    coeffs = (1.0 / 120.0, 26.0 / 120.0, 66.0 / 120.0, 26.0 / 120.0, 1.0 / 120.0)
    real_part = 0.0
    imag_part = 0.0
    for j in range(5):
        angle = ((index * j) % length).astype(jnp.float32) * (2.0 * math.pi / length)
        real_part = real_part + coeffs[j] * jnp.cos(angle)
        imag_part = imag_part + coeffs[j] * jnp.sin(angle)
    return real_part * real_part + imag_part * imag_part


def influence(index_x, index_y, index_z):
    freq_x = jnp.where(2 * index_x < KX, index_x, index_x - KX).astype(jnp.float32) / KX
    freq_y = jnp.where(2 * index_y < KY, index_y, index_y - KY).astype(jnp.float32) / KY
    freq_z = jnp.where(2 * index_z < KZ, index_z, index_z - KZ).astype(jnp.float32) / KZ
    square = freq_x * freq_x + freq_y * freq_y + freq_z * freq_z
    safe = jnp.where(square > 0, square, 1.0)
    volume = float(KX * KY * KZ)
    value = jnp.exp(-(math.pi ** 2) * safe / (ewald_split ** 2)) / (math.pi * volume * safe)
    value = value / (modulus(index_x, KX) * modulus(index_y, KY) * modulus(index_z, KZ))
    return jnp.where(square > 0, value, 0.0)


def reference(cell_offsets, cell_z, frac, charges, tile_counts):
    tiles_x = KX // N_GRP // 2
    tiles_y = KY // N_PEN // 2
    rows_x = KX // 2
    rows_y = KY // 2
    highest = lax.Precision.HIGHEST

    def arrange(arr):
        lead = arr.shape[:-1]
        count = len(lead)
        shaped = arr.reshape(lead + (N_GRP, N_PEN, tiles_x, tiles_y, SLOTS))
        order = tuple(range(count)) + (count, count + 2, count + 1, count + 3, count + 4)
        return jnp.transpose(shaped, order).reshape(lead + (rows_x, rows_y, SLOTS))

    offsets = jnp.moveaxis(arrange(cell_offsets), 1, 0)
    fracs = jnp.moveaxis(arrange(frac), 1, 0)
    zcell = arrange(cell_z)
    charge = arrange(charges)
    counts = jnp.transpose(tile_counts.reshape(N_GRP, N_PEN, tiles_x, tiles_y), (0, 2, 1, 3)).reshape(rows_x, rows_y)
    row_ids = jnp.arange(rows_x, dtype=jnp.int32)
    eight = jnp.arange(8, dtype=jnp.int32)

    def spread_row(grid, inputs):
        offs, zrow, frow, qrow, crow, row = inputs
        weight_x, grade_x, weight_y, grade_y, weight_z, grade_z, live_q = tile_weights(offs, zrow, frow, qrow, crow, KZ)
        pair = (weight_x[:, :, None, :] * weight_y[:, None, :, :] * live_q[:, None, None, :]).reshape(rows_y, 64, SLOTS)
        spread = jnp.einsum("tfs,tsz->tfz", pair, weight_z, precision=highest).reshape(rows_y, 8, 4, 2, KZ)
        slab = 0.0
        for j in range(4):
            part = jnp.transpose(spread[:, :, j], (1, 0, 2, 3))
            slab = slab + jnp.roll(part, j, axis=1).reshape(8, KY, KZ)
        targets = (2 * row + eight) % KX
        return grid.at[targets].add(slab), None

    start = jnp.zeros((KX, KY, KZ), jnp.float32)
    charge_mesh, _ = lax.scan(spread_row, start, (offsets, zcell, fracs, charge, counts, row_ids))
    spectrum = jnp.fft.fftn(charge_mesh)
    index_x = jnp.arange(KX, dtype=jnp.int32)[:, None, None]
    index_y = jnp.arange(KY, dtype=jnp.int32)[None, :, None]
    index_z = jnp.arange(KZ, dtype=jnp.int32)[None, None, :]
    kernel = influence(index_x, index_y, index_z)
    power = jnp.real(spectrum) ** 2 + jnp.imag(spectrum) ** 2
    energy = 0.5 * jnp.sum(kernel * power)
    potential = jnp.real(jnp.fft.ifftn(kernel * spectrum)) * float(KX * KY * KZ)

    def interp_row(carry, inputs):
        offs, zrow, frow, qrow, crow, row = inputs
        weight_x, grade_x, weight_y, grade_y, weight_z, grade_z, live_q = tile_weights(offs, zrow, frow, qrow, crow, KZ)
        rows = jnp.take(potential, (2 * row + eight) % KX, axis=0)
        parts = []
        for j in range(4):
            parts.append(jnp.roll(rows, -2 * j, axis=1).reshape(8, rows_y, 2, KZ))
        footing = jnp.transpose(jnp.stack(parts, axis=0), (2, 1, 0, 3, 4)).reshape(rows_y, 64, KZ)
        main = jnp.einsum("tfz,tsz->tfs", footing, weight_z, precision=highest).reshape(rows_y, 8, 8, SLOTS)
        tilt = jnp.einsum("tfz,tsz->tfs", footing, grade_z, precision=highest).reshape(rows_y, 8, 8, SLOTS)
        force_x = -live_q * jnp.einsum("txs,tys,txys->ts", grade_x, weight_y, main, precision=highest)
        force_y = -live_q * jnp.einsum("txs,tys,txys->ts", weight_x, grade_y, main, precision=highest)
        force_z = -live_q * jnp.einsum("txs,tys,txys->ts", weight_x, weight_y, tilt, precision=highest)
        return carry, jnp.stack([force_x, force_y, force_z], axis=0)

    _, stacked = lax.scan(interp_row, 0.0, (offsets, zcell, fracs, charge, counts, row_ids))
    forces = stacked.reshape(N_GRP, tiles_x, 3, N_PEN, tiles_y, SLOTS)
    forces = jnp.transpose(forces, (2, 0, 3, 1, 4, 5)).reshape(3, ATOMS)
    return forces, (energy / ATOMS).astype(jnp.float32)
```

```python
import functools
import math

import jax
import jax.numpy as jnp
import numpy as np
from jax import lax
from jax.experimental import pallas as pl
from jax.experimental.pallas import tpu as pltpu
from jax.sharding import PartitionSpec as P

K = 256
ATOMS = 1048576
EWALD_SPLIT = 0.6
AXES = ("grp", "pen")
N_GRP = 8
N_PEN = 32
BLOCK_X = K // N_GRP
BLOCK_Y = K // N_PEN
TILES_X = BLOCK_X // 2
PAD_X = BLOCK_X + 5
PAD_Y = BLOCK_Y + 5
USED = PAD_X * PAD_Y
CHUNK = 512
ROWS = 16 * (2 * TILES_X + 6)
ROW_X = 40
F32 = jnp.float32
BF16 = jnp.bfloat16


def halves(table):
    high = table.astype(np.float32).astype(jnp.bfloat16)
    low = (table - high.astype(np.float64)).astype(np.float32).astype(jnp.bfloat16)
    return high, low


def cas(rows, columns):
    angle = (np.outer(rows, columns) % K) * (2.0 * math.pi / K)
    return np.cos(angle) + np.sin(angle)


def make_tables():
    index = np.arange(K)
    full = cas(index, index)
    spread_y = (BLOCK_Y * np.arange(N_PEN)[None, :] + np.arange(16)[:, None]).reshape(-1)
    valid_y = np.repeat(np.arange(16) < PAD_Y, N_PEN)
    table_y = cas(spread_y, index) * valid_y[:, None]
    spread_x = (BLOCK_X * np.arange(N_GRP)[:, None] + np.arange(ROW_X)[None, :]).reshape(-1)
    valid_x = np.tile(np.arange(ROW_X) < PAD_X, N_GRP)
    table_x = cas(index, spread_x) * valid_x[None, :]
    frequency = np.where(2 * index < K, index, index - K) / K
    square = frequency * frequency
    coeffs = np.array([1.0, 26.0, 66.0, 26.0, 1.0]) / 120.0
    phase = np.exp(2j * math.pi * np.outer(index, np.arange(5)) / K)
    modulus = np.abs(phase @ coeffs) ** 2
    factor = np.exp(-(math.pi**2) * square / EWALD_SPLIT**2) / modulus
    plane_factor = np.outer(factor, factor) / (math.pi * float(K) ** 3)
    plane_square = square[:, None] + square[None, :]
    lone = np.stack([factor, square])
    return dict(
        full=halves(full),
        y=halves(table_y),
        x=halves(table_x),
        xt=halves(table_x.T),
        factor=plane_factor.astype(np.float32),
        square=plane_square.astype(np.float32),
        lone=lone.astype(np.float32),
    )


TABLES = make_tables()


def split(value):
    high = value.astype(BF16)
    low = (value - high.astype(F32)).astype(BF16)
    return high, low


def dot(left, right, dims=((1,), (0,))):
    return lax.dot_general(left, right, (dims, ((), ())), preferred_element_type=F32)


def dot3(left, right, dims=((1,), (0,))):
    return (
        dot(left[0], right[0], dims) + dot(left[1], right[0], dims) + dot(left[0], right[1], dims)
    )


def spline_rows(fracs):
    values = [jnp.ones_like(fracs)]
    fifth = values
    for order in range(2, 7):
        scale = 1.0 / (order - 1)
        nxt = []
        for j in range(order):
            term = None
            if j >= 1:
                term = values[j - 1] * ((fracs + float(order - 1 - j)) * scale)
            if j <= order - 2:
                part = values[j] * ((float(1 + j) - fracs) * scale)
                term = part if term is None else term + part
            nxt.append(term)
        if order == 5:
            fifth = nxt
        values = nxt
    slopes = []
    for j in range(6):
        if j == 0:
            slopes.append(-fifth[0])
        elif j == 5:
            slopes.append(fifth[4])
        else:
            slopes.append(fifth[j - 1] - fifth[j])
    return values, slopes


def iota(shape, axis):
    return lax.broadcasted_iota(jnp.int32, shape, axis)


def pick(distance, rows):
    value = jnp.zeros(distance.shape, F32)
    for j in range(6):
        value = jnp.where(distance == j, rows[j], value)
    return value


def column_parts(column, counts_ref, offsets_ref, cell_z_ref, frac_ref, charges_ref):
    lanes = pl.ds(pl.multiple_of(column * 256, 256), 256)
    values, slopes = spline_rows(frac_ref[:, lanes])
    lane = iota((1, 256), 1)
    tile = lane // 64
    counts = jnp.full((1, 256), counts_ref[4 * column], jnp.int32)
    for b in range(1, 4):
        counts = jnp.where(tile == b, counts_ref[4 * column + b], counts)
    live_q = jnp.where(lane % 64 < counts, charges_ref[:, lanes], 0.0)
    rows = [[value[d : d + 1, :] for value in values] for d in range(3)]
    grades = [[slope[d : d + 1, :] for slope in slopes] for d in range(3)]
    from_x = iota((8, 256), 0) - offsets_ref[0:1, lanes]
    from_y = iota((16, 256), 0) - (offsets_ref[1:2, lanes] + 2 * tile)
    from_z = (iota((256, 256), 0) - cell_z_ref[:, lanes]) & (K - 1)
    return lanes, live_q, rows, grades, from_x, from_y, from_z


def spread_kernel(
    counts_ref, offsets_ref, cell_z_ref, frac_ref, charges_ref, high_ref, low_ref, out_ref,
    mesh_ref, packed_ref,
):
    mesh_ref[...] = jnp.zeros_like(mesh_ref)

    @pl.loop(0, TILES_X)
    def _(column):
        lanes, live_q, rows, grades, from_x, from_y, from_z = column_parts(
            column, counts_ref, offsets_ref, cell_z_ref, frac_ref, charges_ref
        )
        weight_x = pick(from_x, rows[0]) * live_q
        weight_y = pick(from_y, rows[1])
        pair = jnp.concatenate([weight_x[i : i + 1, :] * weight_y for i in range(8)], axis=0)
        weight_z = pick(from_z, rows[2])
        part = dot3(split(pair), split(weight_z), ((1,), (1,)))
        place = pl.ds(pl.multiple_of(column * 32, 32), 128)
        for h in range(2):
            mesh_ref[h, place, :] += part[:, 128 * h : 128 * h + 128]

    for y in range(PAD_Y):
        for h in range(2):
            packed_ref[PAD_X * y : PAD_X * (y + 1), 128 * h : 128 * h + 128] = mesh_ref[
                h, pl.ds(y, PAD_X, stride=16), :
            ]
    packed_ref[USED:, :] = jnp.zeros((CHUNK - USED, 256), F32)
    spectrum = dot3((high_ref[...], low_ref[...]), split(packed_ref[...]), ((1,), (1,)))
    for j in range(4):
        out_ref[pl.ds(j, 256, stride=4), :] = spectrum[:, 128 * j : 128 * j + 128]


def plane_kernel(
    lone_ref, in_ref, factor_ref, square_ref, yh_ref, yl_ref, xh_ref, xl_ref, xth_ref, xtl_ref,
    out_ref, turned_ref, wide_ref,
):
    for j in range(4):
        turned = in_ref[pl.ds(j, 256, stride=4), :].T
        for h in range(2):
            turned_ref[h, 128 * j : 128 * j + 128, :] = turned[:, 128 * h : 128 * h + 128]
    section = iota((ROW_X, 128), 1) // 32
    for g in range(N_GRP):
        for quad in range(4):
            block = jnp.zeros((ROW_X, 128), F32)
            for s in range(4):
                y = 4 * quad + s
                if y < PAD_Y:
                    piece = turned_ref[g // 4, PAD_X * y : PAD_X * y + ROW_X, :]
                    shift = (32 * (s - g % 4)) % 128
                    if shift:
                        piece = pltpu.roll(piece, shift, 1)
                    block = jnp.where(section == s, piece, block)
            wide_ref[ROW_X * g : ROW_X * (g + 1), 128 * quad : 128 * quad + 128] = block
    table_y = (yh_ref[...], yl_ref[...])
    half = dot3(split(wide_ref[...]), table_y)
    spectrum = dot3((xh_ref[...], xl_ref[...]), split(half))
    mode = lax.axis_index("grp") * N_PEN + lax.axis_index("pen")
    square = square_ref[...] + lone_ref[1, mode]
    nonzero = square > 0
    kernel = jnp.where(
        nonzero, factor_ref[...] * lone_ref[0, mode] / jnp.where(nonzero, square, 1.0), 0.0
    )
    scaled = kernel * spectrum
    energy = jnp.sum(jnp.sum(scaled * spectrum, axis=0, keepdims=True), axis=1, keepdims=True)
    energy = energy * (0.5 / ATOMS)
    back = dot3((xth_ref[...], xtl_ref[...]), split(scaled))
    wide_ref[...] = dot3(split(back), table_y, ((1,), (1,)))
    for y in range(PAD_Y):
        for h in range(2):
            block = jnp.zeros((ROW_X, 128), F32)
            for s in range(4):
                g = 4 * h + s
                piece = wide_ref[
                    ROW_X * g : ROW_X * (g + 1), 128 * (y // 4) : 128 * (y // 4) + 128
                ]
                shift = (32 * (s - y % 4)) % 128
                if shift:
                    piece = pltpu.roll(piece, shift, 1)
                block = jnp.where(section == s, piece, block)
            turned_ref[h, PAD_X * y : PAD_X * (y + 1), :] = block[:PAD_X]
    lane = iota((256, 128), 1)
    for h in range(2):
        turned_ref[h, USED:CHUNK, :] = jnp.zeros((CHUNK - USED, 128), F32)
    for j in range(4):
        rows = slice(128 * j, 128 * j + 128)
        block = jnp.concatenate([turned_ref[0, rows, :], turned_ref[1, rows, :]], axis=1).T
        if j == 3:
            block = jnp.where(lane == USED - 384, energy, block)
        out_ref[pl.ds(j, 256, stride=4), :] = block


def force_kernel(
    counts_ref, offsets_ref, cell_z_ref, frac_ref, charges_ref, in_ref, high_ref, low_ref,
    forces_ref, energy_ref, packed_ref, mesh_ref, mesh_high_ref, mesh_low_ref,
):
    table = (high_ref[...], low_ref[...])
    lane = iota((256, 128), 1)
    for j in range(4):
        chunk = in_ref[pl.ds(j, 256, stride=4), :]
        if j == 3:
            energies = jnp.where(lane == USED - 384, chunk, 0.0)
            energy_ref[...] = jnp.sum(
                jnp.sum(energies, axis=0, keepdims=True), axis=1, keepdims=True
            )
        packed_ref[128 * j : 128 * j + 128, :] = dot3(split(chunk.T), table)
    mesh_ref[...] = jnp.zeros_like(mesh_ref)
    for y in range(PAD_Y):
        for h in range(2):
            mesh_ref[h, pl.ds(y, PAD_X, stride=16), :] = packed_ref[
                PAD_X * y : PAD_X * (y + 1), 128 * h : 128 * h + 128
            ]
    for h in range(2):
        high, low = split(mesh_ref[h])
        mesh_high_ref[:, 128 * h : 128 * h + 128] = high
        mesh_low_ref[:, 128 * h : 128 * h + 128] = low

    @pl.loop(0, TILES_X)
    def _(column):
        lanes, live_q, rows, grades, from_x, from_y, from_z = column_parts(
            column, counts_ref, offsets_ref, cell_z_ref, frac_ref, charges_ref
        )
        weight_x = pick(from_x, rows[0])
        grade_x = pick(from_x, grades[0])
        weight_y = pick(from_y, rows[1])
        grade_y = pick(from_y, grades[1])
        place = pl.ds(pl.multiple_of(column * 32, 32), 128)
        footing = (mesh_high_ref[place, :], mesh_low_ref[place, :])
        main = dot3(footing, split(pick(from_z, rows[2])))
        tilt = dot3(footing, split(pick(from_z, grades[2])))
        along_x = 0.0
        along_y = 0.0
        along_z = 0.0
        for i in range(8):
            band = main[16 * i : 16 * i + 16, :]
            along_x = along_x + grade_x[i : i + 1, :] * band
            along_y = along_y + weight_x[i : i + 1, :] * band
            along_z = along_z + weight_x[i : i + 1, :] * tilt[16 * i : 16 * i + 16, :]
        forces_ref[0:1, lanes] = -live_q * jnp.sum(weight_y * along_x, axis=0, keepdims=True)
        forces_ref[1:2, lanes] = -live_q * jnp.sum(grade_y * along_y, axis=0, keepdims=True)
        forces_ref[2:3, lanes] = -live_q * jnp.sum(weight_y * along_z, axis=0, keepdims=True)


def call(kernel, out_shape, scratch, *args):
    specs = [
        pl.BlockSpec(memory_space=pltpu.SMEM if name == "s" else pltpu.VMEM) for name, _ in args
    ]
    vmem = pl.BlockSpec(memory_space=pltpu.VMEM)
    return pl.pallas_call(
        kernel,
        out_shape=out_shape,
        in_specs=specs,
        out_specs=jax.tree.map(lambda _: vmem, out_shape),
        scratch_shapes=scratch,
    )(*[value for _, value in args])


def exchange(block):
    return lax.all_to_all(block.reshape(256, 4, 128), AXES, 0, 0, tiled=True).reshape(1024, 128)


def local(cell_offsets, cell_z, frac, charges, tile_counts):
    slots = charges.shape[0]
    high, low = TABLES["full"]
    atoms = [
        ("s", tile_counts),
        ("v", cell_offsets),
        ("v", cell_z.reshape(1, slots)),
        ("v", frac),
        ("v", charges.reshape(1, slots)),
    ]
    table = [("v", jnp.asarray(high)), ("v", jnp.asarray(low))]
    block = jax.ShapeDtypeStruct((1024, 128), F32)
    outgoing = call(
        spread_kernel,
        block,
        [pltpu.VMEM((2, ROWS, 128), F32), pltpu.VMEM((CHUNK, 256), F32)],
        *atoms,
        *table,
    )
    plane = exchange(outgoing)
    planes = [TABLES["factor"], TABLES["square"], *TABLES["y"], *TABLES["x"], *TABLES["xt"]]
    returning = call(
        plane_kernel,
        block,
        [pltpu.VMEM((2, CHUNK, 128), F32), pltpu.VMEM((N_GRP * ROW_X, CHUNK), F32)],
        ("s", jnp.asarray(TABLES["lone"])),
        ("v", plane),
        *[("v", jnp.asarray(value)) for value in planes],
    )
    home = exchange(returning)
    forces, energy = call(
        force_kernel,
        (jax.ShapeDtypeStruct((3, slots), F32), jax.ShapeDtypeStruct((1, 1), F32)),
        [
            pltpu.VMEM((CHUNK, 256), F32),
            pltpu.VMEM((2, ROWS, 128), F32),
            pltpu.VMEM((ROWS, 256), BF16),
            pltpu.VMEM((ROWS, 256), BF16),
        ],
        *atoms,
        ("v", home),
        *table,
    )
    return forces, energy.reshape(())


def solution(mesh):
    return jax.shard_map(
        local,
        mesh=mesh,
        in_specs=(P(None, AXES), P(AXES), P(None, AXES), P(AXES), P(AXES)),
        out_specs=(P(None, AXES), P()),
        check_vma=False,
    )
```

```python
import functools
import math

import jax
import jax.numpy as jnp
import numpy as np
from jax import lax
from jax.experimental import pallas as pl
from jax.experimental.pallas import tpu as pltpu
from jax.sharding import PartitionSpec as P

K = 256
ATOMS = 1048576
EWALD_SPLIT = 0.6
AXES = ("grp", "pen")
N_GRP = 8
N_PEN = 32
BLOCK_X = K // N_GRP
BLOCK_Y = K // N_PEN
TILES_X = BLOCK_X // 2
PAD_X = BLOCK_X + 5
PAD_Y = BLOCK_Y + 5
USED = PAD_X * PAD_Y
CHUNK = 512
ROWS = 16 * (2 * TILES_X + 6)
ROW_X = 40
F32 = jnp.float32
BF16 = jnp.bfloat16


def halves(table):
    high = table.astype(np.float32).astype(jnp.bfloat16)
    low = (table - high.astype(np.float64)).astype(np.float32).astype(jnp.bfloat16)
    return high, low


def cas(rows, columns):
    angle = (np.outer(rows, columns) % K) * (2.0 * math.pi / K)
    return np.cos(angle) + np.sin(angle)


def make_tables():
    index = np.arange(K)
    full = cas(index, index)
    spread_y = (BLOCK_Y * np.arange(N_PEN)[None, :] + np.arange(16)[:, None]).reshape(-1)
    valid_y = np.repeat(np.arange(16) < PAD_Y, N_PEN)
    table_y = cas(spread_y, index) * valid_y[:, None]
    spread_x = (BLOCK_X * np.arange(N_GRP)[:, None] + np.arange(ROW_X)[None, :]).reshape(-1)
    valid_x = np.tile(np.arange(ROW_X) < PAD_X, N_GRP)
    table_x = cas(index, spread_x) * valid_x[None, :]
    frequency = np.where(2 * index < K, index, index - K) / K
    square = frequency * frequency
    coeffs = np.array([1.0, 26.0, 66.0, 26.0, 1.0]) / 120.0
    phase = np.exp(2j * math.pi * np.outer(index, np.arange(5)) / K)
    modulus = np.abs(phase @ coeffs) ** 2
    factor = np.exp(-(math.pi**2) * square / EWALD_SPLIT**2) / modulus
    plane_factor = np.outer(factor, factor) / (math.pi * float(K) ** 3)
    plane_square = square[:, None] + square[None, :]
    lone = np.stack([factor, square])
    return dict(
        full=halves(full),
        y=halves(table_y),
        x=halves(table_x),
        xt=halves(table_x.T),
        factor=plane_factor.astype(np.float32),
        square=plane_square.astype(np.float32),
        lone=lone.astype(np.float32),
    )


TABLES = make_tables()


def split(value):
    high = value.astype(BF16)
    low = (value - high.astype(F32)).astype(BF16)
    return high, low


def dot(left, right, dims=((1,), (0,))):
    return lax.dot_general(left, right, (dims, ((), ())), preferred_element_type=F32)


def dot3(left, right, dims=((1,), (0,))):
    return (
        dot(left[0], right[0], dims) + dot(left[1], right[0], dims) + dot(left[0], right[1], dims)
    )


def spline_rows(fracs):
    values = [jnp.ones_like(fracs)]
    fifth = values
    for order in range(2, 7):
        scale = 1.0 / (order - 1)
        nxt = []
        for j in range(order):
            term = None
            if j >= 1:
                term = values[j - 1] * ((fracs + float(order - 1 - j)) * scale)
            if j <= order - 2:
                part = values[j] * ((float(1 + j) - fracs) * scale)
                term = part if term is None else term + part
            nxt.append(term)
        if order == 5:
            fifth = nxt
        values = nxt
    slopes = []
    for j in range(6):
        if j == 0:
            slopes.append(-fifth[0])
        elif j == 5:
            slopes.append(fifth[4])
        else:
            slopes.append(fifth[j - 1] - fifth[j])
    return values, slopes


def iota(shape, axis):
    return lax.broadcasted_iota(jnp.int32, shape, axis)


def pick(distance, rows):
    value = jnp.zeros(distance.shape, F32)
    for j in range(6):
        value = jnp.where(distance == j, rows[j], value)
    return value


def column_parts(column, counts_ref, offsets_ref, cell_z_ref, frac_ref, charges_ref):
    lanes = pl.ds(pl.multiple_of(column * 256, 256), 256)
    values, slopes = spline_rows(frac_ref[:, lanes])
    lane = iota((1, 256), 1)
    tile = lane // 64
    counts = jnp.full((1, 256), counts_ref[4 * column], jnp.int32)
    for b in range(1, 4):
        counts = jnp.where(tile == b, counts_ref[4 * column + b], counts)
    live_q = jnp.where(lane % 64 < counts, charges_ref[:, lanes], 0.0)
    rows = [[value[d : d + 1, :] for value in values] for d in range(3)]
    grades = [[slope[d : d + 1, :] for slope in slopes] for d in range(3)]
    from_x = iota((8, 256), 0) - offsets_ref[0:1, lanes]
    from_y = iota((16, 256), 0) - (offsets_ref[1:2, lanes] + 2 * tile)
    cell_z = cell_z_ref[:, lanes]
    from_z = (iota((16, 256), 0) - cell_z) & 15
    owner_z = (((cell_z + from_z) & (K - 1)) >> 4).astype(F32).astype(BF16)
    return lanes, live_q, rows, grades, from_x, from_y, from_z, owner_z


def along_z(from_z, owner_z, rows):
    zero = jnp.zeros((16, 256), BF16)
    parts = split(pick(from_z, rows))
    return tuple(
        jnp.concatenate([jnp.where(owner_z == float(h), part, zero) for h in range(16)], axis=0)
        for part in parts
    )


def spread_kernel(
    counts_ref, offsets_ref, cell_z_ref, frac_ref, charges_ref, high_ref, low_ref, out_ref,
    mesh_ref, packed_ref,
):
    mesh_ref[...] = jnp.zeros_like(mesh_ref)

    @pl.loop(0, TILES_X, unroll=4)
    def _(column):
        lanes, live_q, rows, grades, from_x, from_y, from_z, owner_z = column_parts(
            column, counts_ref, offsets_ref, cell_z_ref, frac_ref, charges_ref
        )
        weight_x = pick(from_x, rows[0]) * live_q
        weight_y = pick(from_y, rows[1])
        pair = jnp.concatenate([weight_x[i : i + 1, :] * weight_y for i in range(8)], axis=0)
        weight_z = along_z(from_z, owner_z, rows[2])
        part = dot3(split(pair), weight_z, ((1,), (1,)))
        place = pl.ds(pl.multiple_of(column * 32, 32), 128)
        for h in range(2):
            mesh_ref[h, place, :] += part[:, 128 * h : 128 * h + 128]

    for y in range(PAD_Y):
        for h in range(2):
            packed_ref[PAD_X * y : PAD_X * (y + 1), 128 * h : 128 * h + 128] = mesh_ref[
                h, pl.ds(y, PAD_X, stride=16), :
            ]
    packed_ref[USED:, :] = jnp.zeros((CHUNK - USED, 256), F32)
    spectrum = dot3((high_ref[...], low_ref[...]), split(packed_ref[...]), ((1,), (1,)))
    for j in range(4):
        out_ref[pl.ds(j, 256, stride=4), :] = spectrum[:, 128 * j : 128 * j + 128]


def plane_kernel(
    lone_ref, in_ref, factor_ref, square_ref, yh_ref, yl_ref, xh_ref, xl_ref, xth_ref, xtl_ref,
    out_ref, turned_ref, wide_ref,
):
    for j in range(4):
        turned = in_ref[pl.ds(j, 256, stride=4), :].T
        for h in range(2):
            turned_ref[h, 128 * j : 128 * j + 128, :] = turned[:, 128 * h : 128 * h + 128]
    section = iota((ROW_X, 128), 1) // 32
    for g in range(N_GRP):
        for quad in range(4):
            block = jnp.zeros((ROW_X, 128), F32)
            for s in range(4):
                y = 4 * quad + s
                if y < PAD_Y:
                    piece = turned_ref[g // 4, PAD_X * y : PAD_X * y + ROW_X, :]
                    shift = (32 * (s - g % 4)) % 128
                    if shift:
                        piece = pltpu.roll(piece, shift, 1)
                    block = jnp.where(section == s, piece, block)
            wide_ref[ROW_X * g : ROW_X * (g + 1), 128 * quad : 128 * quad + 128] = block
    table_y = (yh_ref[...], yl_ref[...])
    half = dot3(split(wide_ref[...]), table_y)
    spectrum = dot3((xh_ref[...], xl_ref[...]), split(half))
    mode = lax.axis_index("grp") * N_PEN + lax.axis_index("pen")
    square = square_ref[...] + lone_ref[1, mode]
    nonzero = square > 0
    kernel = jnp.where(
        nonzero, factor_ref[...] * lone_ref[0, mode] / jnp.where(nonzero, square, 1.0), 0.0
    )
    scaled = kernel * spectrum
    energy = jnp.sum(jnp.sum(scaled * spectrum, axis=0, keepdims=True), axis=1, keepdims=True)
    energy = energy * (0.5 / ATOMS)
    back = dot3((xth_ref[...], xtl_ref[...]), split(scaled))
    wide_ref[...] = dot3(split(back), table_y, ((1,), (1,)))
    for y in range(PAD_Y):
        for h in range(2):
            block = jnp.zeros((ROW_X, 128), F32)
            for s in range(4):
                g = 4 * h + s
                piece = wide_ref[
                    ROW_X * g : ROW_X * (g + 1), 128 * (y // 4) : 128 * (y // 4) + 128
                ]
                shift = (32 * (s - y % 4)) % 128
                if shift:
                    piece = pltpu.roll(piece, shift, 1)
                block = jnp.where(section == s, piece, block)
            turned_ref[h, PAD_X * y : PAD_X * (y + 1), :] = block[:PAD_X]
    lane = iota((256, 128), 1)
    for h in range(2):
        turned_ref[h, USED:CHUNK, :] = jnp.zeros((CHUNK - USED, 128), F32)
    for j in range(4):
        rows = slice(128 * j, 128 * j + 128)
        block = jnp.concatenate([turned_ref[0, rows, :], turned_ref[1, rows, :]], axis=1).T
        if j == 3:
            block = jnp.where(lane == USED - 384, energy, block)
        out_ref[pl.ds(j, 256, stride=4), :] = block


def force_kernel(
    counts_ref, offsets_ref, cell_z_ref, frac_ref, charges_ref, in_ref, high_ref, low_ref,
    forces_ref, energy_ref, packed_ref, mesh_ref, mesh_high_ref, mesh_low_ref,
):
    table = (high_ref[...], low_ref[...])
    lane = iota((256, 128), 1)
    for j in range(4):
        chunk = in_ref[pl.ds(j, 256, stride=4), :]
        if j == 3:
            energies = jnp.where(lane == USED - 384, chunk, 0.0)
            energy_ref[...] = jnp.sum(
                jnp.sum(energies, axis=0, keepdims=True), axis=1, keepdims=True
            )
        packed_ref[128 * j : 128 * j + 128, :] = dot3(split(chunk.T), table)
    mesh_ref[...] = jnp.zeros_like(mesh_ref)
    for y in range(PAD_Y):
        for h in range(2):
            mesh_ref[h, pl.ds(y, PAD_X, stride=16), :] = packed_ref[
                PAD_X * y : PAD_X * (y + 1), 128 * h : 128 * h + 128
            ]
    for h in range(2):
        high, low = split(mesh_ref[h])
        mesh_high_ref[:, 128 * h : 128 * h + 128] = high
        mesh_low_ref[:, 128 * h : 128 * h + 128] = low

    @pl.loop(0, TILES_X, unroll=4)
    def _(column):
        lanes, live_q, rows, grades, from_x, from_y, from_z, owner_z = column_parts(
            column, counts_ref, offsets_ref, cell_z_ref, frac_ref, charges_ref
        )
        weight_x = pick(from_x, rows[0])
        grade_x = pick(from_x, grades[0])
        weight_y = pick(from_y, rows[1])
        grade_y = pick(from_y, grades[1])
        place = pl.ds(pl.multiple_of(column * 32, 32), 128)
        footing = (mesh_high_ref[place, :], mesh_low_ref[place, :])
        main = dot3(footing, along_z(from_z, owner_z, rows[2]))
        tilt = dot3(footing, along_z(from_z, owner_z, grades[2]))
        sum_x = 0.0
        sum_y = 0.0
        sum_z = 0.0
        for i in range(8):
            band = main[16 * i : 16 * i + 16, :]
            sum_x = sum_x + grade_x[i : i + 1, :] * band
            sum_y = sum_y + weight_x[i : i + 1, :] * band
            sum_z = sum_z + weight_x[i : i + 1, :] * tilt[16 * i : 16 * i + 16, :]
        forces_ref[0:1, lanes] = -live_q * jnp.sum(weight_y * sum_x, axis=0, keepdims=True)
        forces_ref[1:2, lanes] = -live_q * jnp.sum(grade_y * sum_y, axis=0, keepdims=True)
        forces_ref[2:3, lanes] = -live_q * jnp.sum(weight_y * sum_z, axis=0, keepdims=True)


def call(kernel, out_shape, scratch, *args):
    specs = [
        pl.BlockSpec(memory_space=pltpu.SMEM if name == "s" else pltpu.VMEM) for name, _ in args
    ]
    vmem = pl.BlockSpec(memory_space=pltpu.VMEM)
    return pl.pallas_call(
        kernel,
        out_shape=out_shape,
        in_specs=specs,
        out_specs=jax.tree.map(lambda _: vmem, out_shape),
        scratch_shapes=scratch,
        compiler_params=pltpu.CompilerParams(vmem_limit_bytes=16 * 1024 * 1024),
    )(*[value for _, value in args])


def exchange(block):
    return lax.all_to_all(block.reshape(256, 4, 128), AXES, 0, 0, tiled=True).reshape(1024, 128)


def local(cell_offsets, cell_z, frac, charges, tile_counts):
    slots = charges.shape[0]
    high, low = TABLES["full"]
    atoms = [
        ("s", tile_counts),
        ("v", cell_offsets),
        ("v", cell_z.reshape(1, slots)),
        ("v", frac),
        ("v", charges.reshape(1, slots)),
    ]
    table = [("v", jnp.asarray(high)), ("v", jnp.asarray(low))]
    block = jax.ShapeDtypeStruct((1024, 128), F32)
    outgoing = call(
        spread_kernel,
        block,
        [pltpu.VMEM((2, ROWS, 128), F32), pltpu.VMEM((CHUNK, 256), F32)],
        *atoms,
        *table,
    )
    plane = exchange(outgoing)
    planes = [TABLES["factor"], TABLES["square"], *TABLES["y"], *TABLES["x"], *TABLES["xt"]]
    returning = call(
        plane_kernel,
        block,
        [pltpu.VMEM((2, CHUNK, 128), F32), pltpu.VMEM((N_GRP * ROW_X, CHUNK), F32)],
        ("s", jnp.asarray(TABLES["lone"])),
        ("v", plane),
        *[("v", jnp.asarray(value)) for value in planes],
    )
    home = exchange(returning)
    forces, energy = call(
        force_kernel,
        (jax.ShapeDtypeStruct((3, slots), F32), jax.ShapeDtypeStruct((1, 1), F32)),
        [
            pltpu.VMEM((CHUNK, 256), F32),
            pltpu.VMEM((2, ROWS, 128), F32),
            pltpu.VMEM((ROWS, 256), BF16),
            pltpu.VMEM((ROWS, 256), BF16),
        ],
        *atoms,
        ("v", home),
        *table,
    )
    return forces, energy.reshape(())


def solution(mesh):
    return jax.shard_map(
        local,
        mesh=mesh,
        in_specs=(P(None, AXES), P(AXES), P(None, AXES), P(AXES), P(AXES)),
        out_specs=(P(None, AXES), P()),
        check_vma=False,
    )
```

```python
import functools
import math

import jax
import jax.numpy as jnp
import numpy as np
from jax import lax
from jax.experimental import pallas as pl
from jax.experimental.pallas import tpu as pltpu
from jax.sharding import PartitionSpec as P

K = 256
ATOMS = 1048576
EWALD_SPLIT = 0.6
AXES = ("grp", "pen")
N_GRP = 8
N_PEN = 32
BLOCK_X = K // N_GRP
BLOCK_Y = K // N_PEN
TILES_X = BLOCK_X // 2
PAD_X = BLOCK_X + 5
PAD_Y = BLOCK_Y + 5
USED = PAD_X * PAD_Y
CHUNK = 512
ROWS = 16 * (2 * TILES_X + 6)
ROW_X = 40
SPARE = 16
F32 = jnp.float32
BF16 = jnp.bfloat16


def halves(table):
    high = table.astype(np.float32).astype(jnp.bfloat16)
    low = (table - high.astype(np.float64)).astype(np.float32).astype(jnp.bfloat16)
    return high, low


def cas(rows, columns):
    angle = (np.outer(rows, columns) % K) * (2.0 * math.pi / K)
    return np.cos(angle) + np.sin(angle)


def make_tables():
    index = np.arange(K)
    full = cas(index, index)
    spread_y = (BLOCK_Y * np.arange(N_PEN)[None, :] + np.arange(16)[:, None]).reshape(-1)
    valid_y = np.repeat(np.arange(16) < PAD_Y, N_PEN)
    table_y = cas(spread_y, index) * valid_y[:, None]
    spread_x = (BLOCK_X * np.arange(N_GRP)[:, None] + np.arange(ROW_X)[None, :]).reshape(-1)
    valid_x = np.tile(np.arange(ROW_X) < PAD_X, N_GRP)
    table_x = cas(index, spread_x) * valid_x[None, :]
    frequency = np.where(2 * index < K, index, index - K) / K
    square = frequency * frequency
    coeffs = np.array([1.0, 26.0, 66.0, 26.0, 1.0]) / 120.0
    phase = np.exp(2j * math.pi * np.outer(index, np.arange(5)) / K)
    modulus = np.abs(phase @ coeffs) ** 2
    factor = np.exp(-(math.pi**2) * square / EWALD_SPLIT**2) / modulus
    plane_factor = np.outer(factor, factor) / (math.pi * float(K) ** 3)
    plane_square = square[:, None] + square[None, :]
    lone = np.stack([factor, square])
    return dict(
        full=halves(full),
        y=halves(table_y),
        x=halves(table_x),
        xt=halves(table_x.T),
        factor=plane_factor.astype(np.float32),
        square=plane_square.astype(np.float32),
        lone=lone.astype(np.float32),
    )


TABLES = make_tables()


def split(value):
    high = value.astype(BF16)
    low = (value - high.astype(F32)).astype(BF16)
    return high, low


def dot(left, right, dims=((1,), (0,))):
    return lax.dot_general(left, right, (dims, ((), ())), preferred_element_type=F32)


def dot3(left, right, dims=((1,), (0,))):
    return (
        dot(left[0], right[0], dims) + dot(left[1], right[0], dims) + dot(left[0], right[1], dims)
    )


def spline_rows(fracs):
    values = [jnp.ones_like(fracs)]
    fifth = values
    for order in range(2, 7):
        scale = 1.0 / (order - 1)
        nxt = []
        for j in range(order):
            term = None
            if j >= 1:
                term = values[j - 1] * ((fracs + float(order - 1 - j)) * scale)
            if j <= order - 2:
                part = values[j] * ((float(1 + j) - fracs) * scale)
                term = part if term is None else term + part
            nxt.append(term)
        if order == 5:
            fifth = nxt
        values = nxt
    slopes = []
    for j in range(6):
        if j == 0:
            slopes.append(-fifth[0])
        elif j == 5:
            slopes.append(fifth[4])
        else:
            slopes.append(fifth[j - 1] - fifth[j])
    return values, slopes


def iota(shape, axis):
    return lax.broadcasted_iota(jnp.int32, shape, axis)


def pick(distance, rows):
    value = jnp.zeros(distance.shape, F32)
    for j in range(6):
        value = jnp.where(distance == j, rows[j], value)
    return value


def column_parts(column, offsets_ref, cell_z_ref, frac_ref):
    lanes = pl.ds(pl.multiple_of(column * 256, 256), 256)
    values, slopes = spline_rows(frac_ref[:, lanes])
    tile = iota((1, 256), 1) // 64
    rows = [[value[d : d + 1, :] for value in values] for d in range(3)]
    grades = [[slope[d : d + 1, :] for slope in slopes] for d in range(3)]
    from_x = iota((8, 256), 0) - offsets_ref[0:1, lanes]
    from_y = iota((16, 256), 0) - (offsets_ref[1:2, lanes] + 2 * tile)
    cell_z = cell_z_ref[:, lanes]
    from_z = (iota((16, 256), 0) - cell_z) & 15
    owner_z = (((cell_z + from_z) & (K - 1)) >> 4).astype(F32).astype(BF16)
    return lanes, rows, grades, from_x, from_y, from_z, owner_z


def along_z(from_z, owner_z, rows):
    zero = jnp.zeros((16, 256), BF16)
    parts = split(pick(from_z, rows))
    return tuple(
        jnp.concatenate([jnp.where(owner_z == float(h), part, zero) for h in range(16)], axis=0)
        for part in parts
    )


def spread_kernel(
    counts_hbm, offsets_hbm, cell_z_hbm, frac_hbm, charges_hbm, high_hbm, low_hbm, out_ref, live_ref,
    mesh_ref, packed_ref, counts_ref, offsets_ref, cell_z_ref, frac_ref, charges_ref, high_ref,
    low_ref, sems,
):
    sources = [counts_hbm, offsets_hbm, cell_z_hbm, frac_hbm, charges_hbm, high_hbm, low_hbm]
    targets = [counts_ref, offsets_ref, cell_z_ref, frac_ref, charges_ref, high_ref, low_ref]
    copies = [
        pltpu.make_async_copy(source, target, sems.at[i])
        for i, (source, target) in enumerate(zip(sources, targets))
    ]
    for copy in copies:
        copy.start()
    mesh_ref[...] = jnp.zeros_like(mesh_ref)
    for copy in copies[:5]:
        copy.wait()

    @pl.loop(0, TILES_X, unroll=4)
    def _(column):
        lanes, rows, grades, from_x, from_y, from_z, owner_z = column_parts(
            column, offsets_ref, cell_z_ref, frac_ref
        )
        lane = iota((1, 256), 1)
        counts = jnp.full((1, 256), counts_ref[4 * column], jnp.int32)
        for b in range(1, 4):
            counts = jnp.where(lane // 64 == b, counts_ref[4 * column + b], counts)
        live_q = jnp.where(lane % 64 < counts, charges_ref[:, lanes], 0.0)
        live_ref[:, lanes] = live_q
        weight_x = pick(from_x, rows[0]) * live_q
        weight_y = pick(from_y, rows[1])
        pair = jnp.concatenate([weight_x[i : i + 1, :] * weight_y for i in range(8)], axis=0)
        weight_z = along_z(from_z, owner_z, rows[2])
        place = pl.ds(pl.multiple_of(column * 32, 32), 128)
        mesh_ref[place, :] += dot3(split(pair), weight_z, ((1,), (1,)))

    for x in range(PAD_X):
        packed_ref[PAD_Y * x : PAD_Y * (x + 1), :] = mesh_ref[16 * x : 16 * x + PAD_Y, :]
    packed_ref[USED:, :] = jnp.zeros((CHUNK - USED, 256), F32)
    for copy in copies[5:]:
        copy.wait()
    spectrum = dot3((high_ref[...], low_ref[...]), split(packed_ref[...]), ((1,), (1,)))
    for j in range(4):
        out_ref[pl.ds(j, 256, stride=4), :] = spectrum[:, 128 * j : 128 * j + 128]


def plane_kernel(
    lone_ref, in_ref, factor_ref, square_ref, yh_ref, yl_ref, xh_ref, xl_ref, xth_ref, xtl_ref,
    out_ref, turned_ref, wide_ref,
):
    for j in range(4):
        turned = in_ref[pl.ds(j, 256, stride=4), :].T
        for h in range(2):
            turned_ref[h, 128 * j : 128 * j + 128, :] = turned[:, 128 * h : 128 * h + 128]
    turned_ref[:, CHUNK:, :] = jnp.zeros((2, SPARE, 128), F32)
    section = iota((ROW_X, 128), 1) // 32
    for g in range(N_GRP):
        for quad in range(4):
            block = jnp.zeros((ROW_X, 128), F32)
            for s in range(4):
                y = 4 * quad + s
                if y < PAD_Y:
                    piece = turned_ref[g // 4, pl.ds(y, ROW_X, stride=PAD_Y), :]
                    shift = (32 * (s - g % 4)) % 128
                    if shift:
                        piece = pltpu.roll(piece, shift, 1)
                    block = jnp.where(section == s, piece, block)
            wide_ref[ROW_X * g : ROW_X * (g + 1), 128 * quad : 128 * quad + 128] = block
    table_y = (yh_ref[...], yl_ref[...])
    half = dot3(split(wide_ref[...]), table_y)
    spectrum = dot3((xh_ref[...], xl_ref[...]), split(half))
    mode = lax.axis_index("grp") * N_PEN + lax.axis_index("pen")
    lone = jnp.where(iota((2, 256), 1) == mode, lone_ref[...], 0.0)
    lone = jnp.sum(lone, axis=1, keepdims=True)
    square = square_ref[...] + lone[1:2, :]
    nonzero = square > 0
    kernel = jnp.where(
        nonzero, factor_ref[...] * lone[0:1, :] / jnp.where(nonzero, square, 1.0), 0.0
    )
    scaled = kernel * spectrum
    energy = jnp.sum(jnp.sum(scaled * spectrum, axis=0, keepdims=True), axis=1, keepdims=True)
    energy = energy * (0.5 / ATOMS)
    back = dot3((xth_ref[...], xtl_ref[...]), split(scaled))
    wide_ref[...] = dot3(split(back), table_y, ((1,), (1,)))
    for y in range(PAD_Y):
        for h in range(2):
            block = jnp.zeros((ROW_X, 128), F32)
            for s in range(4):
                g = 4 * h + s
                piece = wide_ref[
                    ROW_X * g : ROW_X * (g + 1), 128 * (y // 4) : 128 * (y // 4) + 128
                ]
                shift = (32 * (s - y % 4)) % 128
                if shift:
                    piece = pltpu.roll(piece, shift, 1)
                block = jnp.where(section == s, piece, block)
            turned_ref[h, pl.ds(y, PAD_X, stride=PAD_Y), :] = block[:PAD_X]
    lane = iota((256, 128), 1)
    for h in range(2):
        turned_ref[h, USED:CHUNK, :] = jnp.zeros((CHUNK - USED, 128), F32)
    for j in range(4):
        rows = slice(128 * j, 128 * j + 128)
        block = jnp.concatenate([turned_ref[0, rows, :], turned_ref[1, rows, :]], axis=1).T
        if j == 3:
            block = jnp.where(lane == USED - 384, energy, block)
        out_ref[pl.ds(j, 256, stride=4), :] = block


def force_kernel(
    offsets_ref, cell_z_ref, frac_ref, live_ref, in_ref, high_ref, low_ref, forces_ref, energy_ref,
    packed_ref, mesh_high_ref, mesh_low_ref,
):
    table = (high_ref[...], low_ref[...])
    lane = iota((256, 128), 1)
    for j in range(4):
        chunk = in_ref[pl.ds(j, 256, stride=4), :]
        if j == 3:
            energies = jnp.where(lane == USED - 384, chunk, 0.0)
            energy_ref[...] = jnp.sum(
                jnp.sum(energies, axis=0, keepdims=True), axis=1, keepdims=True
            )
        packed_ref[128 * j : 128 * j + 128, :] = dot3(split(chunk.T), table)
    for x in range(PAD_X):
        high, low = split(packed_ref[PAD_Y * x : PAD_Y * x + 16, :])
        mesh_high_ref[16 * x : 16 * x + 16, :] = high
        mesh_low_ref[16 * x : 16 * x + 16, :] = low
    mesh_high_ref[16 * PAD_X :, :] = jnp.zeros((ROWS - 16 * PAD_X, 256), BF16)
    mesh_low_ref[16 * PAD_X :, :] = jnp.zeros((ROWS - 16 * PAD_X, 256), BF16)

    @pl.loop(0, TILES_X, unroll=4)
    def _(column):
        lanes, rows, grades, from_x, from_y, from_z, owner_z = column_parts(
            column, offsets_ref, cell_z_ref, frac_ref
        )
        live_q = live_ref[:, lanes]
        weight_x = pick(from_x, rows[0])
        grade_x = pick(from_x, grades[0])
        weight_y = pick(from_y, rows[1])
        grade_y = pick(from_y, grades[1])
        place = pl.ds(pl.multiple_of(column * 32, 32), 128)
        footing = (mesh_high_ref[place, :], mesh_low_ref[place, :])
        main = dot3(footing, along_z(from_z, owner_z, rows[2]))
        tilt = dot3(footing, along_z(from_z, owner_z, grades[2]))
        sum_x = 0.0
        sum_y = 0.0
        sum_z = 0.0
        for i in range(8):
            band = main[16 * i : 16 * i + 16, :]
            sum_x = sum_x + grade_x[i : i + 1, :] * band
            sum_y = sum_y + weight_x[i : i + 1, :] * band
            sum_z = sum_z + weight_x[i : i + 1, :] * tilt[16 * i : 16 * i + 16, :]
        forces_ref[0:1, lanes] = -live_q * jnp.sum(weight_y * sum_x, axis=0, keepdims=True)
        forces_ref[1:2, lanes] = -live_q * jnp.sum(grade_y * sum_y, axis=0, keepdims=True)
        forces_ref[2:3, lanes] = -live_q * jnp.sum(weight_y * sum_z, axis=0, keepdims=True)


def call(kernel, out_shape, scratch, *args, memory=pltpu.VMEM):
    vmem = pl.BlockSpec(memory_space=pltpu.VMEM)
    return pl.pallas_call(
        kernel,
        out_shape=out_shape,
        in_specs=[pl.BlockSpec(memory_space=memory)] * len(args),
        out_specs=jax.tree.map(lambda _: vmem, out_shape),
        scratch_shapes=scratch,
        compiler_params=pltpu.CompilerParams(vmem_limit_bytes=16 * 1024 * 1024),
    )(*args)


def exchange(block):
    return lax.all_to_all(block.reshape(256, 4, 128), AXES, 0, 0, tiled=True).reshape(1024, 128)


def local(cell_offsets, cell_z, frac, charges, tile_counts):
    slots = charges.shape[0]
    cell_z = cell_z.reshape(1, slots)
    charges = charges.reshape(1, slots)
    table = [jnp.asarray(value) for value in TABLES["full"]]
    block = jax.ShapeDtypeStruct((1024, 128), F32)
    sources = [tile_counts, cell_offsets, cell_z, frac, charges, *table]
    outgoing, live_q = call(
        spread_kernel,
        (block, jax.ShapeDtypeStruct((1, slots), F32)),
        [
            pltpu.VMEM((ROWS, 256), F32),
            pltpu.VMEM((CHUNK, 256), F32),
            pltpu.SMEM(tile_counts.shape, jnp.int32),
            *[pltpu.VMEM(source.shape, source.dtype) for source in sources[1:]],
            pltpu.SemaphoreType.DMA((len(sources),)),
        ],
        *[pltpu.with_memory_space_constraint(source, pltpu.HBM) for source in sources],
        memory=pltpu.HBM,
    )
    plane = exchange(outgoing)
    planes = [TABLES["factor"], TABLES["square"], *TABLES["y"], *TABLES["x"], *TABLES["xt"]]
    returning = call(
        plane_kernel,
        block,
        [pltpu.VMEM((2, CHUNK + SPARE, 128), F32), pltpu.VMEM((N_GRP * ROW_X, CHUNK), F32)],
        jnp.asarray(TABLES["lone"]),
        plane,
        *[jnp.asarray(value) for value in planes],
    )
    home = exchange(returning)
    forces, energy = call(
        force_kernel,
        (jax.ShapeDtypeStruct((3, slots), F32), jax.ShapeDtypeStruct((1, 1), F32)),
        [
            pltpu.VMEM((CHUNK, 256), F32),
            pltpu.VMEM((ROWS, 256), BF16),
            pltpu.VMEM((ROWS, 256), BF16),
        ],
        cell_offsets,
        cell_z,
        frac,
        live_q,
        home,
        *table,
    )
    return forces, energy.reshape(())


def solution(mesh):
    return jax.shard_map(
        local,
        mesh=mesh,
        in_specs=(P(None, AXES), P(AXES), P(None, AXES), P(AXES), P(AXES)),
        out_specs=(P(None, AXES), P()),
        check_vma=False,
    )
```

```python
import functools
import math

import jax
import jax.numpy as jnp
import numpy as np
from jax import lax
from jax.experimental import pallas as pl
from jax.experimental.pallas import tpu as pltpu
from jax.sharding import PartitionSpec as P

K = 256
ATOMS = 1048576
EWALD_SPLIT = 0.6
AXES = ("grp", "pen")
N_GRP = 8
N_PEN = 32
BLOCK_X = K // N_GRP
BLOCK_Y = K // N_PEN
TILES_X = BLOCK_X // 2
PAD_X = BLOCK_X + 5
PAD_Y = BLOCK_Y + 5
USED = PAD_X * PAD_Y
CHUNK = 512
ROWS = 16 * (2 * TILES_X + 6)
ROW_X = 40
SPARE = 16
GROUP = 4
F32 = jnp.float32
BF16 = jnp.bfloat16


def halves(table):
    high = table.astype(np.float32).astype(jnp.bfloat16)
    low = (table - high.astype(np.float64)).astype(np.float32).astype(jnp.bfloat16)
    return high, low


def cas(rows, columns):
    angle = (np.outer(rows, columns) % K) * (2.0 * math.pi / K)
    return np.cos(angle) + np.sin(angle)


def make_tables():
    index = np.arange(K)
    full = cas(index, index)
    spread_y = (BLOCK_Y * np.arange(N_PEN)[None, :] + np.arange(16)[:, None]).reshape(-1)
    valid_y = np.repeat(np.arange(16) < PAD_Y, N_PEN)
    table_y = cas(spread_y, index) * valid_y[:, None]
    spread_x = (BLOCK_X * np.arange(N_GRP)[:, None] + np.arange(ROW_X)[None, :]).reshape(-1)
    valid_x = np.tile(np.arange(ROW_X) < PAD_X, N_GRP)
    table_x = cas(index, spread_x) * valid_x[None, :]
    frequency = np.where(2 * index < K, index, index - K) / K
    square = frequency * frequency
    coeffs = np.array([1.0, 26.0, 66.0, 26.0, 1.0]) / 120.0
    phase = np.exp(2j * math.pi * np.outer(index, np.arange(5)) / K)
    modulus = np.abs(phase @ coeffs) ** 2
    factor = np.exp(-(math.pi**2) * square / EWALD_SPLIT**2) / modulus
    plane_factor = np.outer(factor, factor) / (math.pi * float(K) ** 3)
    plane_square = square[:, None] + square[None, :]
    lone = np.stack([factor, square])
    return dict(
        full=halves(full),
        wide=np.concatenate([*halves(table_y), *halves(table_x.T)]),
        x=np.concatenate(halves(table_x)),
        plane=np.concatenate([plane_factor, plane_square, lone]).astype(np.float32),
    )


TABLES = make_tables()


def split(value):
    high = value.astype(BF16)
    low = (value - high.astype(F32)).astype(BF16)
    return high, low


def dot(left, right, dims=((1,), (0,))):
    return lax.dot_general(left, right, (dims, ((), ())), preferred_element_type=F32)


def dot3(left, right, dims=((1,), (0,))):
    size = left[0].shape[0]
    both = dot(jnp.concatenate(left, axis=0), right[0], dims)
    return both[:size] + both[size:] + dot(left[0], right[1], dims)


def spline_rows(fracs):
    values = [jnp.ones_like(fracs)]
    fifth = values
    for order in range(2, 7):
        scale = 1.0 / (order - 1)
        nxt = []
        for j in range(order):
            term = None
            if j >= 1:
                term = values[j - 1] * ((fracs + float(order - 1 - j)) * scale)
            if j <= order - 2:
                part = values[j] * ((float(1 + j) - fracs) * scale)
                term = part if term is None else term + part
            nxt.append(term)
        if order == 5:
            fifth = nxt
        values = nxt
    slopes = []
    for j in range(6):
        if j == 0:
            slopes.append(-fifth[0])
        elif j == 5:
            slopes.append(fifth[4])
        else:
            slopes.append(fifth[j - 1] - fifth[j])
    return values, slopes


def iota(shape, axis):
    return lax.broadcasted_iota(jnp.int32, shape, axis)


def pick(distance, rows):
    value = jnp.zeros(distance.shape, F32)
    for j in range(6):
        value = jnp.where(distance == j, rows[j], value)
    return value


def column_lanes(column):
    return pl.ds(pl.multiple_of(column * 256, 256), 256)


def group_splines(group, frac_ref):
    fracs = [frac_ref[:, column_lanes(GROUP * group + c)] for c in range(GROUP)]
    return spline_rows(jnp.concatenate(fracs, axis=0))


def column_parts(group, c, splines, offsets_ref, cell_z_ref):
    column = GROUP * group + c
    lanes = column_lanes(column)
    rows, grades = [
        [[value[3 * c + d : 3 * c + d + 1, :] for value in values] for d in range(3)]
        for values in splines
    ]
    tile = iota((1, 256), 1) // 64
    from_x = iota((8, 256), 0) - offsets_ref[0:1, lanes]
    from_y = iota((16, 256), 0) - (offsets_ref[1:2, lanes] + 2 * tile)
    cell_z = cell_z_ref[:, lanes]
    from_z = (iota((16, 256), 0) - cell_z) & 15
    owner_z = (((cell_z + from_z) & (K - 1)) >> 4).astype(F32).astype(BF16)
    return column, lanes, rows, grades, from_x, from_y, from_z, owner_z


def along_z(from_z, owner_z, rows):
    zero = jnp.zeros((16, 256), BF16)
    parts = split(pick(from_z, rows))
    return tuple(
        jnp.concatenate([jnp.where(owner_z == float(h), part, zero) for h in range(16)], axis=0)
        for part in parts
    )


def spread_kernel(
    counts_hbm, offsets_hbm, cell_z_hbm, frac_hbm, charges_hbm, high_hbm, low_hbm, out_ref, live_ref,
    mesh_ref, packed_ref, counts_ref, offsets_ref, cell_z_ref, frac_ref, charges_ref, high_ref,
    low_ref, sems,
):
    sources = [counts_hbm, offsets_hbm, cell_z_hbm, frac_hbm, charges_hbm, high_hbm, low_hbm]
    targets = [counts_ref, offsets_ref, cell_z_ref, frac_ref, charges_ref, high_ref, low_ref]
    copies = [
        pltpu.make_async_copy(source, target, sems.at[i])
        for i, (source, target) in enumerate(zip(sources, targets))
    ]
    for copy in copies:
        copy.start()
    mesh_ref[...] = jnp.zeros_like(mesh_ref)
    for copy in copies[:5]:
        copy.wait()

    @pl.loop(0, TILES_X // GROUP)
    def _(group):
        splines = group_splines(group, frac_ref)
        for c in range(GROUP):
            column, lanes, rows, grades, from_x, from_y, from_z, owner_z = column_parts(
                group, c, splines, offsets_ref, cell_z_ref
            )
            lane = iota((1, 256), 1)
            counts = jnp.full((1, 256), counts_ref[4 * column], jnp.int32)
            for b in range(1, 4):
                counts = jnp.where(lane // 64 == b, counts_ref[4 * column + b], counts)
            live_q = jnp.where(lane % 64 < counts, charges_ref[:, lanes], 0.0)
            live_ref[:, lanes] = live_q
            weight_x = pick(from_x, rows[0]) * live_q
            weight_y = pick(from_y, rows[1])
            pair = jnp.concatenate([weight_x[i : i + 1, :] * weight_y for i in range(8)], axis=0)
            weight_z = along_z(from_z, owner_z, rows[2])
            place = pl.ds(pl.multiple_of(column * 32, 32), 128)
            mesh_ref[place, :] += dot3(split(pair), weight_z, ((1,), (1,)))

    for x in range(PAD_X):
        packed_ref[PAD_Y * x : PAD_Y * (x + 1), :] = mesh_ref[16 * x : 16 * x + PAD_Y, :]
    packed_ref[USED:, :] = jnp.zeros((CHUNK - USED, 256), F32)
    for copy in copies[5:]:
        copy.wait()
    spectrum = dot3((high_ref[...], low_ref[...]), split(packed_ref[...]), ((1,), (1,)))
    for j in range(4):
        out_ref[pl.ds(j, 256, stride=4), :] = spectrum[:, 128 * j : 128 * j + 128]


def plane_kernel(
    in_ref, plane_ref, table_ref, x_ref, out_ref, turned_ref, wide_ref
):
    for j in range(4):
        turned = in_ref[pl.ds(j, 256, stride=4), :].T
        for h in range(2):
            turned_ref[h, 128 * j : 128 * j + 128, :] = turned[:, 128 * h : 128 * h + 128]
    turned_ref[:, CHUNK:, :] = jnp.zeros((2, SPARE, 128), F32)
    section = iota((ROW_X, 128), 1) // 32
    for g in range(N_GRP):
        for quad in range(4):
            block = jnp.zeros((ROW_X, 128), F32)
            for s in range(4):
                y = 4 * quad + s
                if y < PAD_Y:
                    piece = turned_ref[g // 4, pl.ds(y, ROW_X, stride=PAD_Y), :]
                    shift = (32 * (s - g % 4)) % 128
                    if shift:
                        piece = pltpu.roll(piece, shift, 1)
                    block = jnp.where(section == s, piece, block)
            wide_ref[ROW_X * g : ROW_X * (g + 1), 128 * quad : 128 * quad + 128] = block
    table_y = (table_ref[:CHUNK, :], table_ref[CHUNK : 2 * CHUNK, :])
    table_xt = (table_ref[2 * CHUNK : 2 * CHUNK + 320, :], table_ref[2 * CHUNK + 320 :, :])
    half = dot3(split(wide_ref[...]), table_y)
    spectrum = dot3((x_ref[:K, :], x_ref[K:, :]), split(half))
    mode = lax.axis_index("grp") * N_PEN + lax.axis_index("pen")
    lone = jnp.where(iota((2, 256), 1) == mode, plane_ref[2 * K :, :], 0.0)
    lone = jnp.sum(lone, axis=1, keepdims=True)
    square = plane_ref[K : 2 * K, :] + lone[1:2, :]
    nonzero = square > 0
    kernel = jnp.where(
        nonzero, plane_ref[:K, :] * lone[0:1, :] / jnp.where(nonzero, square, 1.0), 0.0
    )
    scaled = kernel * spectrum
    energy = jnp.sum(jnp.sum(scaled * spectrum, axis=0, keepdims=True), axis=1, keepdims=True)
    energy = energy * (0.5 / ATOMS)
    back = dot3(table_xt, split(scaled))
    wide_ref[...] = dot3(split(back), table_y, ((1,), (1,)))
    for y in range(PAD_Y):
        for h in range(2):
            block = jnp.zeros((ROW_X, 128), F32)
            for s in range(4):
                g = 4 * h + s
                piece = wide_ref[
                    ROW_X * g : ROW_X * (g + 1), 128 * (y // 4) : 128 * (y // 4) + 128
                ]
                shift = (32 * (s - y % 4)) % 128
                if shift:
                    piece = pltpu.roll(piece, shift, 1)
                block = jnp.where(section == s, piece, block)
            turned_ref[h, pl.ds(y, PAD_X, stride=PAD_Y), :] = block[:PAD_X]
    lane = iota((256, 128), 1)
    for h in range(2):
        turned_ref[h, USED:CHUNK, :] = jnp.zeros((CHUNK - USED, 128), F32)
    for j in range(4):
        rows = slice(128 * j, 128 * j + 128)
        block = jnp.concatenate([turned_ref[0, rows, :], turned_ref[1, rows, :]], axis=1).T
        if j == 3:
            block = jnp.where(lane == USED - 384, energy, block)
        out_ref[pl.ds(j, 256, stride=4), :] = block


def force_kernel(
    offsets_ref, cell_z_ref, frac_ref, live_ref, in_ref, high_ref, low_ref, forces_ref, energy_ref,
    packed_ref, mesh_high_ref, mesh_low_ref,
):
    table = (high_ref[...], low_ref[...])
    lane = iota((256, 128), 1)
    for j in range(4):
        chunk = in_ref[pl.ds(j, 256, stride=4), :]
        if j == 3:
            energies = jnp.where(lane == USED - 384, chunk, 0.0)
            energy_ref[...] = jnp.sum(
                jnp.sum(energies, axis=0, keepdims=True), axis=1, keepdims=True
            )
        packed_ref[128 * j : 128 * j + 128, :] = dot3(split(chunk.T), table)
    for x in range(PAD_X):
        high, low = split(packed_ref[PAD_Y * x : PAD_Y * x + 16, :])
        mesh_high_ref[16 * x : 16 * x + 16, :] = high
        mesh_low_ref[16 * x : 16 * x + 16, :] = low
    mesh_high_ref[16 * PAD_X :, :] = jnp.zeros((ROWS - 16 * PAD_X, 256), BF16)
    mesh_low_ref[16 * PAD_X :, :] = jnp.zeros((ROWS - 16 * PAD_X, 256), BF16)

    @pl.loop(0, TILES_X // GROUP)
    def _(group):
        splines = group_splines(group, frac_ref)
        for c in range(GROUP):
            column, lanes, rows, grades, from_x, from_y, from_z, owner_z = column_parts(
                group, c, splines, offsets_ref, cell_z_ref
            )
            live_q = live_ref[:, lanes]
            weight_x = pick(from_x, rows[0])
            grade_x = pick(from_x, grades[0])
            weight_y = pick(from_y, rows[1])
            grade_y = pick(from_y, grades[1])
            place = pl.ds(pl.multiple_of(column * 32, 32), 128)
            footing = (mesh_high_ref[place, :], mesh_low_ref[place, :])
            main = dot3(footing, along_z(from_z, owner_z, rows[2]))
            tilt = dot3(footing, along_z(from_z, owner_z, grades[2]))
            sum_x = 0.0
            sum_y = 0.0
            sum_z = 0.0
            for i in range(8):
                band = main[16 * i : 16 * i + 16, :]
                sum_x = sum_x + grade_x[i : i + 1, :] * band
                sum_y = sum_y + weight_x[i : i + 1, :] * band
                sum_z = sum_z + weight_x[i : i + 1, :] * tilt[16 * i : 16 * i + 16, :]
            forces_ref[0:1, lanes] = -live_q * jnp.sum(weight_y * sum_x, axis=0, keepdims=True)
            forces_ref[1:2, lanes] = -live_q * jnp.sum(grade_y * sum_y, axis=0, keepdims=True)
            forces_ref[2:3, lanes] = -live_q * jnp.sum(weight_y * sum_z, axis=0, keepdims=True)


def call(kernel, out_shape, scratch, *args, memory=pltpu.VMEM):
    vmem = pl.BlockSpec(memory_space=pltpu.VMEM)
    return pl.pallas_call(
        kernel,
        out_shape=out_shape,
        in_specs=[pl.BlockSpec(memory_space=memory)] * len(args),
        out_specs=jax.tree.map(lambda _: vmem, out_shape),
        scratch_shapes=scratch,
        compiler_params=pltpu.CompilerParams(vmem_limit_bytes=8 * 1024 * 1024),
        cost_estimate=pl.CostEstimate(flops=3 * 10**9, bytes_accessed=10**7, transcendentals=0),
    )(*args)


def exchange(block):
    return lax.all_to_all(block.reshape(256, 4, 128), AXES, 0, 0, tiled=True).reshape(1024, 128)


def local(cell_offsets, cell_z, frac, charges, tile_counts):
    slots = charges.shape[0]
    cell_z = cell_z.reshape(1, slots)
    charges = charges.reshape(1, slots)
    table = [jnp.asarray(value) for value in TABLES["full"]]
    block = jax.ShapeDtypeStruct((1024, 128), F32)
    sources = [tile_counts, cell_offsets, cell_z, frac, charges, *table]
    outgoing, live_q = call(
        spread_kernel,
        (block, jax.ShapeDtypeStruct((1, slots), F32)),
        [
            pltpu.VMEM((ROWS, 256), F32),
            pltpu.VMEM((CHUNK, 256), F32),
            pltpu.SMEM(tile_counts.shape, jnp.int32),
            *[pltpu.VMEM(source.shape, source.dtype) for source in sources[1:]],
            pltpu.SemaphoreType.DMA((len(sources),)),
        ],
        *[pltpu.with_memory_space_constraint(source, pltpu.HBM) for source in sources],
        memory=pltpu.HBM,
    )
    plane = exchange(outgoing)
    returning = call(
        plane_kernel,
        block,
        [pltpu.VMEM((2, CHUNK + SPARE, 128), F32), pltpu.VMEM((N_GRP * ROW_X, CHUNK), F32)],
        plane,
        *[jnp.asarray(TABLES[name]) for name in ("plane", "wide", "x")],
    )
    home = exchange(returning)
    forces, energy = call(
        force_kernel,
        (jax.ShapeDtypeStruct((3, slots), F32), jax.ShapeDtypeStruct((1, 1), F32)),
        [
            pltpu.VMEM((CHUNK, 256), F32),
            pltpu.VMEM((ROWS, 256), BF16),
            pltpu.VMEM((ROWS, 256), BF16),
        ],
        cell_offsets,
        cell_z,
        frac,
        live_q,
        home,
        *table,
    )
    return forces, energy.reshape(())


def solution(mesh):
    return jax.shard_map(
        local,
        mesh=mesh,
        in_specs=(P(None, AXES), P(AXES), P(None, AXES), P(AXES), P(AXES)),
        out_specs=(P(None, AXES), P()),
        check_vma=False,
    )
```

```python
import functools
import math

import jax
import jax.numpy as jnp
import numpy as np
from jax import lax
from jax.experimental import pallas as pl
from jax.experimental.pallas import tpu as pltpu
from jax.sharding import PartitionSpec as P

K = 256
ATOMS = 1048576
EWALD_SPLIT = 0.6
AXES = ("grp", "pen")
N_GRP = 8
N_PEN = 32
BLOCK_X = K // N_GRP
BLOCK_Y = K // N_PEN
TILES_X = BLOCK_X // 2
PAD_X = BLOCK_X + 5
PAD_Y = BLOCK_Y + 5
USED = PAD_X * PAD_Y
CHUNK = 512
ROWS = 16 * (2 * TILES_X + 6)
ROW_X = 40
SPARE = 16
GROUP = 16
F32 = jnp.float32
BF16 = jnp.bfloat16


def halves(table):
    high = table.astype(np.float32).astype(jnp.bfloat16)
    low = (table - high.astype(np.float64)).astype(np.float32).astype(jnp.bfloat16)
    return high, low


def cas(rows, columns):
    angle = (np.outer(rows, columns) % K) * (2.0 * math.pi / K)
    return np.cos(angle) + np.sin(angle)


def make_tables():
    index = np.arange(K)
    full = cas(index, index)
    spread_y = (BLOCK_Y * np.arange(N_PEN)[None, :] + np.arange(16)[:, None]).reshape(-1)
    valid_y = np.repeat(np.arange(16) < PAD_Y, N_PEN)
    table_y = cas(spread_y, index) * valid_y[:, None]
    spread_x = (BLOCK_X * np.arange(N_GRP)[:, None] + np.arange(ROW_X)[None, :]).reshape(-1)
    valid_x = np.tile(np.arange(ROW_X) < PAD_X, N_GRP)
    table_x = cas(index, spread_x) * valid_x[None, :]
    frequency = np.where(2 * index < K, index, index - K) / K
    square = frequency * frequency
    coeffs = np.array([1.0, 26.0, 66.0, 26.0, 1.0]) / 120.0
    phase = np.exp(2j * math.pi * np.outer(index, np.arange(5)) / K)
    modulus = np.abs(phase @ coeffs) ** 2
    factor = np.exp(-(math.pi**2) * square / EWALD_SPLIT**2) / modulus
    plane_factor = np.outer(factor, factor) / (math.pi * float(K) ** 3)
    plane_square = square[:, None] + square[None, :]
    lone = np.stack([factor, square])
    return dict(
        full=halves(full),
        wide=np.concatenate([*halves(table_y), *halves(table_x.T)]),
        x=np.concatenate(halves(table_x)),
        plane=np.concatenate([plane_factor, plane_square, lone]).astype(np.float32),
    )


TABLES = make_tables()


def split(value):
    high = value.astype(BF16)
    low = (value - high.astype(F32)).astype(BF16)
    return high, low


def dot(left, right, dims=((1,), (0,))):
    return lax.dot_general(left, right, (dims, ((), ())), preferred_element_type=F32)


def dot3(left, right, dims=((1,), (0,))):
    size = left[0].shape[0]
    both = dot(jnp.concatenate(left, axis=0), right[0], dims)
    return both[:size] + both[size:] + dot(left[0], right[1], dims)


def spline_rows(fracs):
    values = [jnp.ones_like(fracs)]
    fifth = values
    for order in range(2, 7):
        scale = 1.0 / (order - 1)
        nxt = []
        for j in range(order):
            term = None
            if j >= 1:
                term = values[j - 1] * ((fracs + float(order - 1 - j)) * scale)
            if j <= order - 2:
                part = values[j] * ((float(1 + j) - fracs) * scale)
                term = part if term is None else term + part
            nxt.append(term)
        if order == 5:
            fifth = nxt
        values = nxt
    slopes = []
    for j in range(6):
        if j == 0:
            slopes.append(-fifth[0])
        elif j == 5:
            slopes.append(fifth[4])
        else:
            slopes.append(fifth[j - 1] - fifth[j])
    return values, slopes


def iota(shape, axis):
    return lax.broadcasted_iota(jnp.int32, shape, axis)


def pick(distance, rows):
    value = jnp.zeros(distance.shape, F32)
    for j in range(6):
        value = jnp.where(distance == j, rows[j], value)
    return value


def column_lanes(column):
    return pl.ds(pl.multiple_of(column * 256, 256), 256)


def group_splines(group, frac_ref):
    fracs = [frac_ref[:, column_lanes(GROUP * group + c)] for c in range(GROUP)]
    return spline_rows(jnp.concatenate(fracs, axis=0))


def column_parts(group, c, splines, offsets_ref, cell_z_ref):
    column = GROUP * group + c
    lanes = column_lanes(column)
    rows, grades = [
        [[value[3 * c + d : 3 * c + d + 1, :] for value in values] for d in range(3)]
        for values in splines
    ]
    tile = iota((1, 256), 1) // 64
    from_x = iota((8, 256), 0) - offsets_ref[0:1, lanes]
    from_y = iota((16, 256), 0) - (offsets_ref[1:2, lanes] + 2 * tile)
    cell_z = cell_z_ref[:, lanes]
    from_z = (iota((16, 256), 0) - cell_z) & 15
    owner_z = (((cell_z + from_z) & (K - 1)) >> 4).astype(F32).astype(BF16)
    return column, lanes, rows, grades, from_x, from_y, from_z, owner_z


def along_z(from_z, owner_z, rows):
    zero = jnp.zeros((16, 256), BF16)
    parts = split(pick(from_z, rows))
    return tuple(
        jnp.concatenate([jnp.where(owner_z == float(h), part, zero) for h in range(16)], axis=0)
        for part in parts
    )


def spread_kernel(
    counts_hbm, offsets_hbm, cell_z_hbm, frac_hbm, charges_hbm, high_hbm, low_hbm, out_ref, live_ref,
    mesh_ref, packed_ref, counts_ref, offsets_ref, cell_z_ref, frac_ref, charges_ref, high_ref,
    low_ref, sems,
):
    sources = [counts_hbm, offsets_hbm, cell_z_hbm, frac_hbm, charges_hbm, high_hbm, low_hbm]
    targets = [counts_ref, offsets_ref, cell_z_ref, frac_ref, charges_ref, high_ref, low_ref]
    copies = [
        pltpu.make_async_copy(source, target, sems.at[i])
        for i, (source, target) in enumerate(zip(sources, targets))
    ]
    for copy in copies:
        copy.start()
    mesh_ref[...] = jnp.zeros_like(mesh_ref)
    for copy in copies[:5]:
        copy.wait()

    @pl.loop(0, TILES_X // GROUP)
    def _(group):
        splines = group_splines(group, frac_ref)
        for c in range(GROUP):
            column, lanes, rows, grades, from_x, from_y, from_z, owner_z = column_parts(
                group, c, splines, offsets_ref, cell_z_ref
            )
            lane = iota((1, 256), 1)
            counts = jnp.full((1, 256), counts_ref[4 * column], jnp.int32)
            for b in range(1, 4):
                counts = jnp.where(lane // 64 == b, counts_ref[4 * column + b], counts)
            live_q = jnp.where(lane % 64 < counts, charges_ref[:, lanes], 0.0)
            live_ref[:, lanes] = live_q
            weight_x = pick(from_x, rows[0]) * live_q
            weight_y = pick(from_y, rows[1])
            pair = jnp.concatenate([weight_x[i : i + 1, :] * weight_y for i in range(8)], axis=0)
            weight_z = along_z(from_z, owner_z, rows[2])
            place = pl.ds(pl.multiple_of(column * 32, 32), 128)
            mesh_ref[place, :] += dot3(split(pair), weight_z, ((1,), (1,)))

    for x in range(PAD_X):
        packed_ref[PAD_Y * x : PAD_Y * (x + 1), :] = mesh_ref[16 * x : 16 * x + PAD_Y, :]
    packed_ref[USED:, :] = jnp.zeros((CHUNK - USED, 256), F32)
    for copy in copies[5:]:
        copy.wait()
    spectrum = dot3((high_ref[...], low_ref[...]), split(packed_ref[...]), ((1,), (1,)))
    for j in range(4):
        out_ref[pl.ds(j, 256, stride=4), :] = spectrum[:, 128 * j : 128 * j + 128]


def plane_kernel(
    in_ref, plane_ref, table_ref, x_ref, out_ref, turned_ref, wide_ref
):
    for j in range(4):
        turned = in_ref[pl.ds(j, 256, stride=4), :].T
        for h in range(2):
            turned_ref[h, 128 * j : 128 * j + 128, :] = turned[:, 128 * h : 128 * h + 128]
    turned_ref[:, CHUNK:, :] = jnp.zeros((2, SPARE, 128), F32)
    section = iota((ROW_X, 128), 1) // 32
    for g in range(N_GRP):
        for quad in range(4):
            block = jnp.zeros((ROW_X, 128), F32)
            for s in range(4):
                y = 4 * quad + s
                if y < PAD_Y:
                    piece = turned_ref[g // 4, pl.ds(y, ROW_X, stride=PAD_Y), :]
                    shift = (32 * (s - g % 4)) % 128
                    if shift:
                        piece = pltpu.roll(piece, shift, 1)
                    block = jnp.where(section == s, piece, block)
            wide_ref[ROW_X * g : ROW_X * (g + 1), 128 * quad : 128 * quad + 128] = block
    table_y = (table_ref[:CHUNK, :], table_ref[CHUNK : 2 * CHUNK, :])
    table_xt = (table_ref[2 * CHUNK : 2 * CHUNK + 320, :], table_ref[2 * CHUNK + 320 :, :])
    half = dot3(split(wide_ref[...]), table_y)
    spectrum = dot3((x_ref[:K, :], x_ref[K:, :]), split(half))
    mode = lax.axis_index("grp") * N_PEN + lax.axis_index("pen")
    lone = jnp.where(iota((2, 256), 1) == mode, plane_ref[2 * K :, :], 0.0)
    lone = jnp.sum(lone, axis=1, keepdims=True)
    square = plane_ref[K : 2 * K, :] + lone[1:2, :]
    nonzero = square > 0
    kernel = jnp.where(
        nonzero, plane_ref[:K, :] * lone[0:1, :] / jnp.where(nonzero, square, 1.0), 0.0
    )
    scaled = kernel * spectrum
    energy = jnp.sum(jnp.sum(scaled * spectrum, axis=0, keepdims=True), axis=1, keepdims=True)
    energy = energy * (0.5 / ATOMS)
    back = dot3(table_xt, split(scaled))
    wide_ref[...] = dot3(split(back), table_y, ((1,), (1,)))
    for y in range(PAD_Y):
        for h in range(2):
            block = jnp.zeros((ROW_X, 128), F32)
            for s in range(4):
                g = 4 * h + s
                piece = wide_ref[
                    ROW_X * g : ROW_X * (g + 1), 128 * (y // 4) : 128 * (y // 4) + 128
                ]
                shift = (32 * (s - y % 4)) % 128
                if shift:
                    piece = pltpu.roll(piece, shift, 1)
                block = jnp.where(section == s, piece, block)
            turned_ref[h, pl.ds(y, PAD_X, stride=PAD_Y), :] = block[:PAD_X]
    lane = iota((256, 128), 1)
    for h in range(2):
        turned_ref[h, USED:CHUNK, :] = jnp.zeros((CHUNK - USED, 128), F32)
    for j in range(4):
        rows = slice(128 * j, 128 * j + 128)
        block = jnp.concatenate([turned_ref[0, rows, :], turned_ref[1, rows, :]], axis=1).T
        if j == 3:
            block = jnp.where(lane == USED - 384, energy, block)
        out_ref[pl.ds(j, 256, stride=4), :] = block


def force_kernel(
    offsets_ref, cell_z_ref, frac_ref, live_ref, in_ref, high_ref, low_ref, forces_ref, energy_ref,
    packed_ref, mesh_high_ref, mesh_low_ref,
):
    table = (high_ref[...], low_ref[...])
    lane = iota((256, 128), 1)
    for j in range(4):
        chunk = in_ref[pl.ds(j, 256, stride=4), :]
        if j == 3:
            energies = jnp.where(lane == USED - 384, chunk, 0.0)
            energy_ref[...] = jnp.sum(
                jnp.sum(energies, axis=0, keepdims=True), axis=1, keepdims=True
            )
        packed_ref[128 * j : 128 * j + 128, :] = dot3(split(chunk.T), table)
    for x in range(PAD_X):
        high, low = split(packed_ref[PAD_Y * x : PAD_Y * x + 16, :])
        mesh_high_ref[16 * x : 16 * x + 16, :] = high
        mesh_low_ref[16 * x : 16 * x + 16, :] = low
    mesh_high_ref[16 * PAD_X :, :] = jnp.zeros((ROWS - 16 * PAD_X, 256), BF16)
    mesh_low_ref[16 * PAD_X :, :] = jnp.zeros((ROWS - 16 * PAD_X, 256), BF16)

    @pl.loop(0, TILES_X // GROUP)
    def _(group):
        splines = group_splines(group, frac_ref)
        for c in range(GROUP):
            column, lanes, rows, grades, from_x, from_y, from_z, owner_z = column_parts(
                group, c, splines, offsets_ref, cell_z_ref
            )
            live_q = live_ref[:, lanes]
            weight_x = pick(from_x, rows[0])
            grade_x = pick(from_x, grades[0])
            weight_y = pick(from_y, rows[1])
            grade_y = pick(from_y, grades[1])
            place = pl.ds(pl.multiple_of(column * 32, 32), 128)
            footing = (mesh_high_ref[place, :], mesh_low_ref[place, :])
            main = dot3(footing, along_z(from_z, owner_z, rows[2]))
            tilt = dot3(footing, along_z(from_z, owner_z, grades[2]))
            sum_x = 0.0
            sum_y = 0.0
            sum_z = 0.0
            for i in range(8):
                band = main[16 * i : 16 * i + 16, :]
                sum_x = sum_x + grade_x[i : i + 1, :] * band
                sum_y = sum_y + weight_x[i : i + 1, :] * band
                sum_z = sum_z + weight_x[i : i + 1, :] * tilt[16 * i : 16 * i + 16, :]
            forces_ref[0:1, lanes] = -live_q * jnp.sum(weight_y * sum_x, axis=0, keepdims=True)
            forces_ref[1:2, lanes] = -live_q * jnp.sum(grade_y * sum_y, axis=0, keepdims=True)
            forces_ref[2:3, lanes] = -live_q * jnp.sum(weight_y * sum_z, axis=0, keepdims=True)


def call(kernel, out_shape, scratch, *args, memory=pltpu.VMEM):
    vmem = pl.BlockSpec(memory_space=pltpu.VMEM)
    return pl.pallas_call(
        kernel,
        out_shape=out_shape,
        in_specs=[pl.BlockSpec(memory_space=memory)] * len(args),
        out_specs=jax.tree.map(lambda _: vmem, out_shape),
        scratch_shapes=scratch,
        compiler_params=pltpu.CompilerParams(vmem_limit_bytes=8 * 1024 * 1024),
        cost_estimate=pl.CostEstimate(flops=3 * 10**9, bytes_accessed=10**7, transcendentals=0),
    )(*args)


def exchange(block):
    return lax.all_to_all(block.reshape(256, 4, 128), AXES, 0, 0, tiled=True).reshape(1024, 128)


def local(cell_offsets, cell_z, frac, charges, tile_counts):
    slots = charges.shape[0]
    cell_z = cell_z.reshape(1, slots)
    charges = charges.reshape(1, slots)
    table = [jnp.asarray(value) for value in TABLES["full"]]
    block = jax.ShapeDtypeStruct((1024, 128), F32)
    sources = [tile_counts, cell_offsets, cell_z, frac, charges, *table]
    outgoing, live_q = call(
        spread_kernel,
        (block, jax.ShapeDtypeStruct((1, slots), F32)),
        [
            pltpu.VMEM((ROWS, 256), F32),
            pltpu.VMEM((CHUNK, 256), F32),
            pltpu.SMEM(tile_counts.shape, jnp.int32),
            *[pltpu.VMEM(source.shape, source.dtype) for source in sources[1:]],
            pltpu.SemaphoreType.DMA((len(sources),)),
        ],
        *[pltpu.with_memory_space_constraint(source, pltpu.HBM) for source in sources],
        memory=pltpu.HBM,
    )
    plane = exchange(outgoing)
    returning = call(
        plane_kernel,
        block,
        [pltpu.VMEM((2, CHUNK + SPARE, 128), F32), pltpu.VMEM((N_GRP * ROW_X, CHUNK), F32)],
        plane,
        *[jnp.asarray(TABLES[name]) for name in ("plane", "wide", "x")],
    )
    home = exchange(returning)
    forces, energy = call(
        force_kernel,
        (jax.ShapeDtypeStruct((3, slots), F32), jax.ShapeDtypeStruct((1, 1), F32)),
        [
            pltpu.VMEM((CHUNK, 256), F32),
            pltpu.VMEM((ROWS, 256), BF16),
            pltpu.VMEM((ROWS, 256), BF16),
        ],
        cell_offsets,
        cell_z,
        frac,
        live_q,
        home,
        *table,
    )
    return forces, energy.reshape(())


def solution(mesh):
    return jax.shard_map(
        local,
        mesh=mesh,
        in_specs=(P(None, AXES), P(AXES), P(None, AXES), P(AXES), P(AXES)),
        out_specs=(P(None, AXES), P()),
        check_vma=False,
    )
```

```python
import functools
import math

import jax
import jax.numpy as jnp
import numpy as np
from jax import lax
from jax.experimental import pallas as pl
from jax.experimental.pallas import tpu as pltpu
from jax.sharding import PartitionSpec as P

K = 256
ATOMS = 1048576
EWALD_SPLIT = 0.6
AXES = ("grp", "pen")
N_GRP = 8
N_PEN = 32
BLOCK_X = K // N_GRP
BLOCK_Y = K // N_PEN
TILES_X = BLOCK_X // 2
PAD_X = BLOCK_X + 5
PAD_Y = BLOCK_Y + 5
USED = PAD_X * PAD_Y
CHUNK = 512
ROWS = 16 * PAD_X
ROW_X = 40
SPARE = 16
GROUP = 16
F32 = jnp.float32
BF16 = jnp.bfloat16


def halves(table):
    high = table.astype(np.float32).astype(jnp.bfloat16)
    low = (table - high.astype(np.float64)).astype(np.float32).astype(jnp.bfloat16)
    return high, low


def cas(rows, columns):
    angle = (np.outer(rows, columns) % K) * (2.0 * math.pi / K)
    return np.cos(angle) + np.sin(angle)


def make_tables():
    index = np.arange(K)
    full = cas(index, index)
    order_y = (BLOCK_Y * np.arange(N_PEN)[None, :] + np.arange(BLOCK_Y)[:, None]).reshape(-1)
    frequency = np.where(2 * index < K, index, index - K) / K
    square = frequency * frequency
    coeffs = np.array([1.0, 26.0, 66.0, 26.0, 1.0]) / 120.0
    phase = np.exp(2j * math.pi * np.outer(index, np.arange(5)) / K)
    modulus = np.abs(phase @ coeffs) ** 2
    factor = np.exp(-(math.pi**2) * square / EWALD_SPLIT**2) / modulus
    plane_factor = np.outer(factor, factor) / (math.pi * float(K) ** 3)
    plane_square = square[:, None] + square[None, :]
    lone = np.stack([factor, square])
    return dict(
        full=np.concatenate(halves(full)),
        order=np.concatenate(halves(full[order_y])),
        plane=np.concatenate([plane_factor, plane_square, lone]).astype(np.float32),
    )


TABLES = make_tables()


def split(value):
    high = value.astype(BF16)
    low = (value - high.astype(F32)).astype(BF16)
    return high, low


def dot(left, right, dims=((1,), (0,))):
    return lax.dot_general(left, right, (dims, ((), ())), preferred_element_type=F32)


def dot3(left, right, dims=((1,), (0,))):
    size = left[0].shape[0]
    both = dot(jnp.concatenate(left, axis=0), right[0], dims)
    return both[:size] + both[size:] + dot(left[0], right[1], dims)


def spline_rows(fracs):
    values = [jnp.ones_like(fracs)]
    fifth = values
    for order in range(2, 7):
        scale = 1.0 / (order - 1)
        nxt = []
        for j in range(order):
            term = None
            if j >= 1:
                term = values[j - 1] * ((fracs + float(order - 1 - j)) * scale)
            if j <= order - 2:
                part = values[j] * ((float(1 + j) - fracs) * scale)
                term = part if term is None else term + part
            nxt.append(term)
        if order == 5:
            fifth = nxt
        values = nxt
    slopes = []
    for j in range(6):
        if j == 0:
            slopes.append(-fifth[0])
        elif j == 5:
            slopes.append(fifth[4])
        else:
            slopes.append(fifth[j - 1] - fifth[j])
    return values, slopes


def iota(shape, axis):
    return lax.broadcasted_iota(jnp.int32, shape, axis)


def pick(distance, rows):
    value = jnp.zeros(distance.shape, F32)
    for j in range(6):
        value = jnp.where(distance == j, rows[j], value)
    return value


def column_lanes(column):
    return pl.ds(pl.multiple_of(column * 256, 256), 256)


def group_splines(group, frac_ref):
    fracs = [frac_ref[:, column_lanes(GROUP * group + c)] for c in range(GROUP)]
    return spline_rows(jnp.concatenate(fracs, axis=0))


def column_parts(group, c, splines, offsets_ref, cell_z_ref):
    column = GROUP * group + c
    lanes = column_lanes(column)
    rows, grades = [
        [[value[3 * c + d : 3 * c + d + 1, :] for value in values] for d in range(3)]
        for values in splines
    ]
    tile = iota((1, 256), 1) // 64
    from_x = iota((8, 256), 0) - offsets_ref[0:1, lanes]
    from_y = iota((16, 256), 0) - (offsets_ref[1:2, lanes] + 2 * tile)
    cell_z = cell_z_ref[:, lanes]
    from_z = (iota((16, 256), 0) - cell_z) & 15
    owner_z = (((cell_z + from_z) & (K - 1)) >> 4).astype(F32).astype(BF16)
    return column, lanes, rows, grades, from_x, from_y, from_z, owner_z


def along_z(from_z, owner_z, rows):
    zero = jnp.zeros((16, 256), BF16)
    parts = split(pick(from_z, rows))
    return tuple(
        jnp.concatenate([jnp.where(owner_z == float(h), part, zero) for h in range(16)], axis=0)
        for part in parts
    )


def spread_kernel(
    counts_hbm, offsets_hbm, cell_z_hbm, frac_hbm, charges_hbm, table_hbm, out_ref, live_ref,
    mesh_ref, packed_ref, counts_ref, offsets_ref, cell_z_ref, frac_ref, charges_ref, table_ref,
    sems,
):
    sources = [counts_hbm, offsets_hbm, cell_z_hbm, frac_hbm, charges_hbm, table_hbm]
    targets = [counts_ref, offsets_ref, cell_z_ref, frac_ref, charges_ref, table_ref]
    copies = [
        pltpu.make_async_copy(source, target, sems.at[i])
        for i, (source, target) in enumerate(zip(sources, targets))
    ]
    for copy in copies:
        copy.start()
    mesh_ref[...] = jnp.zeros_like(mesh_ref)
    for copy in copies[:5]:
        copy.wait()

    @pl.loop(0, TILES_X // GROUP)
    def _(group):
        splines = group_splines(group, frac_ref)
        for c in range(GROUP):
            column, lanes, rows, grades, from_x, from_y, from_z, owner_z = column_parts(
                group, c, splines, offsets_ref, cell_z_ref
            )
            lane = iota((1, 256), 1)
            counts = jnp.full((1, 256), counts_ref[4 * column], jnp.int32)
            for b in range(1, 4):
                counts = jnp.where(lane // 64 == b, counts_ref[4 * column + b], counts)
            live_q = jnp.where(lane % 64 < counts, charges_ref[:, lanes], 0.0)
            live_ref[:, lanes] = live_q
            weight_x = pick(from_x, rows[0]) * live_q
            weight_y = pick(from_y, rows[1])
            pair = jnp.concatenate([weight_x[i : i + 1, :] * weight_y for i in range(7)], axis=0)
            weight_z = along_z(from_z, owner_z, rows[2])
            place = pl.ds(pl.multiple_of(column * 32, 32), 112)
            mesh_ref[place, :] += dot3(split(pair), weight_z, ((1,), (1,)))

    for x in range(PAD_X):
        packed_ref[PAD_Y * x : PAD_Y * (x + 1), :] = mesh_ref[16 * x : 16 * x + PAD_Y, :]
    packed_ref[USED:, :] = jnp.zeros((CHUNK - USED, 256), F32)
    for copy in copies[5:]:
        copy.wait()
    spectrum = dot3((table_ref[:K, :], table_ref[K:, :]), split(packed_ref[...]), ((1,), (1,)))
    for j in range(4):
        out_ref[pl.ds(j, 256, stride=4), :] = spectrum[:, 128 * j : 128 * j + 128]


def regroup(pieces, own, section):
    block = None
    for s, piece in enumerate(pieces):
        shift = (32 * (s - own)) % 128
        if shift:
            piece = pltpu.roll(piece, shift, 1)
        block = piece if block is None else jnp.where(section == s, piece, block)
    return block


def to_next(value, place):
    return jnp.where(place == 0, pltpu.roll(value, 97, 1), pltpu.roll(value, 1, 1))


def to_previous(value, place):
    return jnp.where(place == 31, pltpu.roll(value, 31, 1), pltpu.roll(value, 127, 1))


def plane_kernel(in_ref, plane_ref, order_ref, table_ref, out_ref, turned_ref, wide_ref):
    for j in range(4):
        turned = in_ref[pl.ds(j, 256, stride=4), :].T
        for h in range(2):
            turned_ref[h, 128 * j : 128 * j + 128, :] = turned[:, 128 * h : 128 * h + 128]
    turned_ref[:, CHUNK:, :] = jnp.zeros((2, SPARE, 128), F32)
    lane = iota((ROW_X, 128), 1)
    section = lane // 32
    place = lane % 32
    merged = []
    for h in range(2):
        lines = [turned_ref[h, pl.ds(y, ROW_X, stride=PAD_Y), :] for y in range(PAD_Y)]
        for y in range(PAD_Y - BLOCK_Y):
            lines[y] = lines[y] + to_next(lines[y + BLOCK_Y], place)
        merged.append(lines[:BLOCK_Y])
    beyond = iota((8, 128), 0) < PAD_X - BLOCK_X
    for quad in range(2):
        blocks = [
            regroup(merged[g // 4][4 * quad : 4 * quad + 4], g % 4, section) for g in range(N_GRP)
        ]
        for g in range(N_GRP):
            halo = jnp.where(beyond, blocks[g - 1][BLOCK_X:], 0.0)
            columns = slice(128 * quad, 128 * quad + 128)
            wide_ref[BLOCK_X * g : BLOCK_X * g + 8, columns] = blocks[g][:8] + halo
            wide_ref[BLOCK_X * g + 8 : BLOCK_X * (g + 1), columns] = blocks[g][8:BLOCK_X]
    order = (order_ref[:K, :], order_ref[K:, :])
    table = (table_ref[:K, :], table_ref[K:, :])
    half = dot3(split(wide_ref[...]), order)
    spectrum = dot3(table, split(half))
    mode = lax.axis_index("grp") * N_PEN + lax.axis_index("pen")
    lone = jnp.where(iota((2, 256), 1) == mode, plane_ref[2 * K :, :], 0.0)
    lone = jnp.sum(lone, axis=1, keepdims=True)
    square = plane_ref[K : 2 * K, :] + lone[1:2, :]
    nonzero = square > 0
    kernel = jnp.where(
        nonzero, plane_ref[:K, :] * lone[0:1, :] / jnp.where(nonzero, square, 1.0), 0.0
    )
    scaled = kernel * spectrum
    energy = jnp.sum(jnp.sum(scaled * spectrum, axis=0, keepdims=True), axis=1, keepdims=True)
    energy = energy * (0.5 / ATOMS)
    back = dot3(table, split(scaled))
    wide_ref[...] = dot3(split(back), order, ((1,), (1,)))
    for h in range(2):
        for quad in range(2):
            columns = slice(128 * quad, 128 * quad + 128)
            pieces = []
            for g in range(4 * h, 4 * h + 4):
                after = BLOCK_X * ((g + 1) % N_GRP)
                pieces.append(
                    jnp.concatenate(
                        [
                            wide_ref[BLOCK_X * g : BLOCK_X * (g + 1), columns],
                            wide_ref[after : after + 8, columns],
                        ],
                        axis=0,
                    )
                )
            for i in range(4):
                y = 4 * quad + i
                block = regroup(pieces, i, section)
                turned_ref[h, pl.ds(y, PAD_X, stride=PAD_Y), :] = block[:PAD_X]
                if y < PAD_Y - BLOCK_Y:
                    block = to_previous(block, place)
                    rows = pl.ds(y + BLOCK_Y, PAD_X, stride=PAD_Y)
                    turned_ref[h, rows, :] = block[:PAD_X]
        turned_ref[h, USED:CHUNK, :] = jnp.zeros((CHUNK - USED, 128), F32)
    spot = iota((256, 128), 1) == USED - 384
    for j in range(4):
        rows = slice(128 * j, 128 * j + 128)
        block = jnp.concatenate([turned_ref[0, rows, :], turned_ref[1, rows, :]], axis=1).T
        if j == 3:
            block = jnp.where(spot, energy, block)
        out_ref[pl.ds(j, 256, stride=4), :] = block


def force_kernel(
    offsets_ref, cell_z_ref, frac_ref, live_ref, in_ref, table_ref, forces_ref, energy_ref,
    packed_ref, mesh_ref, mesh_high_ref, mesh_low_ref,
):
    table = (table_ref[:K, :], table_ref[K:, :])
    lane = iota((256, 128), 1)
    for j in range(4):
        chunk = in_ref[pl.ds(j, 256, stride=4), :]
        if j == 3:
            energies = jnp.where(lane == USED - 384, chunk, 0.0)
            energy_ref[...] = jnp.sum(
                jnp.sum(energies, axis=0, keepdims=True), axis=1, keepdims=True
            )
        packed_ref[128 * j : 128 * j + 128, :] = dot3(split(chunk.T), table)
    for x in range(PAD_X):
        mesh_ref[16 * x : 16 * x + 16, :] = packed_ref[PAD_Y * x : PAD_Y * x + 16, :]
    high, low = split(mesh_ref[...])
    mesh_high_ref[...] = high
    mesh_low_ref[...] = low

    @pl.loop(0, TILES_X // GROUP)
    def _(group):
        splines = group_splines(group, frac_ref)
        for c in range(GROUP):
            column, lanes, rows, grades, from_x, from_y, from_z, owner_z = column_parts(
                group, c, splines, offsets_ref, cell_z_ref
            )
            live_q = live_ref[:, lanes]
            weight_x = pick(from_x, rows[0])
            grade_x = pick(from_x, grades[0])
            weight_y = pick(from_y, rows[1])
            grade_y = pick(from_y, grades[1])
            place = pl.ds(pl.multiple_of(column * 32, 32), 112)
            footing = (mesh_high_ref[place, :], mesh_low_ref[place, :])
            main = dot3(footing, along_z(from_z, owner_z, rows[2]))
            tilt = dot3(footing, along_z(from_z, owner_z, grades[2]))
            sum_x = 0.0
            sum_y = 0.0
            sum_z = 0.0
            for i in range(7):
                band = main[16 * i : 16 * i + 16, :]
                sum_x = sum_x + grade_x[i : i + 1, :] * band
                sum_y = sum_y + weight_x[i : i + 1, :] * band
                sum_z = sum_z + weight_x[i : i + 1, :] * tilt[16 * i : 16 * i + 16, :]
            forces_ref[0:1, lanes] = -live_q * jnp.sum(weight_y * sum_x, axis=0, keepdims=True)
            forces_ref[1:2, lanes] = -live_q * jnp.sum(grade_y * sum_y, axis=0, keepdims=True)
            forces_ref[2:3, lanes] = -live_q * jnp.sum(weight_y * sum_z, axis=0, keepdims=True)


def call(kernel, out_shape, scratch, *args, memory=pltpu.VMEM):
    vmem = pl.BlockSpec(memory_space=pltpu.VMEM)
    return pl.pallas_call(
        kernel,
        out_shape=out_shape,
        in_specs=[pl.BlockSpec(memory_space=memory)] * len(args),
        out_specs=jax.tree.map(lambda _: vmem, out_shape),
        scratch_shapes=scratch,
        compiler_params=pltpu.CompilerParams(vmem_limit_bytes=8 * 1024 * 1024),
        cost_estimate=pl.CostEstimate(flops=3 * 10**9, bytes_accessed=10**7, transcendentals=0),
    )(*args)


def exchange(block):
    return lax.all_to_all(block.reshape(256, 4, 128), AXES, 0, 0, tiled=True).reshape(1024, 128)


def local(cell_offsets, cell_z, frac, charges, tile_counts):
    slots = charges.shape[0]
    cell_z = cell_z.reshape(1, slots)
    charges = charges.reshape(1, slots)
    table = jnp.asarray(TABLES["full"])
    block = jax.ShapeDtypeStruct((1024, 128), F32)
    sources = [tile_counts, cell_offsets, cell_z, frac, charges, table]
    outgoing, live_q = call(
        spread_kernel,
        (block, jax.ShapeDtypeStruct((1, slots), F32)),
        [
            pltpu.VMEM((ROWS, 256), F32),
            pltpu.VMEM((CHUNK, 256), F32),
            pltpu.SMEM(tile_counts.shape, jnp.int32),
            *[pltpu.VMEM(source.shape, source.dtype) for source in sources[1:]],
            pltpu.SemaphoreType.DMA((len(sources),)),
        ],
        *[pltpu.with_memory_space_constraint(source, pltpu.HBM) for source in sources],
        memory=pltpu.HBM,
    )
    plane = exchange(outgoing)
    returning = call(
        plane_kernel,
        block,
        [pltpu.VMEM((2, CHUNK + SPARE, 128), F32), pltpu.VMEM((K, K), F32)],
        plane,
        jnp.asarray(TABLES["plane"]),
        jnp.asarray(TABLES["order"]),
        table,
    )
    home = exchange(returning)
    forces, energy = call(
        force_kernel,
        (jax.ShapeDtypeStruct((3, slots), F32), jax.ShapeDtypeStruct((1, 1), F32)),
        [
            pltpu.VMEM((CHUNK, 256), F32),
            pltpu.VMEM((ROWS, 256), F32),
            pltpu.VMEM((ROWS, 256), BF16),
            pltpu.VMEM((ROWS, 256), BF16),
        ],
        cell_offsets,
        cell_z,
        frac,
        live_q,
        home,
        table,
    )
    return forces, energy.reshape(())


def solution(mesh):
    return jax.shard_map(
        local,
        mesh=mesh,
        in_specs=(P(None, AXES), P(AXES), P(None, AXES), P(AXES), P(AXES)),
        out_specs=(P(None, AXES), P()),
        check_vma=False,
    )
```

```python
import functools
import math

import jax
import jax.numpy as jnp
import numpy as np
from jax import lax
from jax.experimental import pallas as pl
from jax.experimental.pallas import tpu as pltpu
from jax.sharding import PartitionSpec as P

K = 256
ATOMS = 1048576
EWALD_SPLIT = 0.6
AXES = ("grp", "pen")
N_GRP = 8
N_PEN = 32
BLOCK_X = K // N_GRP
BLOCK_Y = K // N_PEN
TILES_X = BLOCK_X // 2
PAD_X = BLOCK_X + 5
PAD_Y = BLOCK_Y + 5
USED = PAD_X * PAD_Y
CHUNK = 512
ROWS = 16 * PAD_X
ROW_X = 40
SPARE = 16
F32 = jnp.float32
BF16 = jnp.bfloat16


def halves(table):
    high = table.astype(np.float32).astype(jnp.bfloat16)
    low = (table - high.astype(np.float64)).astype(np.float32).astype(jnp.bfloat16)
    return high, low


def cas(rows, columns):
    angle = (np.outer(rows, columns) % K) * (2.0 * math.pi / K)
    return np.cos(angle) + np.sin(angle)


def make_tables():
    index = np.arange(K)
    full = cas(index, index)
    order_y = (BLOCK_Y * np.arange(N_PEN)[None, :] + np.arange(BLOCK_Y)[:, None]).reshape(-1)
    frequency = np.where(2 * index < K, index, index - K) / K
    square = frequency * frequency
    coeffs = np.array([1.0, 26.0, 66.0, 26.0, 1.0]) / 120.0
    phase = np.exp(2j * math.pi * np.outer(index, np.arange(5)) / K)
    modulus = np.abs(phase @ coeffs) ** 2
    factor = np.exp(-(math.pi**2) * square / EWALD_SPLIT**2) / modulus
    plane_factor = np.outer(factor, factor) / (math.pi * float(K) ** 3)
    plane_square = square[:, None] + square[None, :]
    lone = np.stack([factor, square])
    return dict(
        full=np.concatenate(halves(full)),
        order=np.concatenate(halves(full[order_y])),
        plane=np.concatenate([plane_factor, plane_square, lone]).astype(np.float32),
    )


TABLES = make_tables()


def split(value):
    high = value.astype(BF16)
    low = (value - high.astype(F32)).astype(BF16)
    return high, low


def dot(left, right, dims=((1,), (0,))):
    return lax.dot_general(left, right, (dims, ((), ())), preferred_element_type=F32)


def dot3(left, right, dims=((1,), (0,))):
    size = left[0].shape[0]
    both = dot(jnp.concatenate(left, axis=0), right[0], dims)
    return both[:size] + both[size:] + dot(left[0], right[1], dims)


def spline_rows(fracs):
    values = [jnp.ones_like(fracs)]
    fifth = values
    for order in range(2, 7):
        scale = 1.0 / (order - 1)
        nxt = []
        for j in range(order):
            term = None
            if j >= 1:
                term = values[j - 1] * ((fracs + float(order - 1 - j)) * scale)
            if j <= order - 2:
                part = values[j] * ((float(1 + j) - fracs) * scale)
                term = part if term is None else term + part
            nxt.append(term)
        if order == 5:
            fifth = nxt
        values = nxt
    slopes = []
    for j in range(6):
        if j == 0:
            slopes.append(-fifth[0])
        elif j == 5:
            slopes.append(fifth[4])
        else:
            slopes.append(fifth[j - 1] - fifth[j])
    return values, slopes


def iota(shape, axis):
    return lax.broadcasted_iota(jnp.int32, shape, axis)


def pick(distance, rows):
    value = jnp.zeros(distance.shape, F32)
    for j in range(6):
        value = jnp.where(distance == j, rows[j], value)
    return value


def column_lanes(column):
    return slice(256 * column, 256 * column + 256)


def group_splines(frac_ref):
    fracs = [frac_ref[:, column_lanes(column)] for column in range(TILES_X)]
    return spline_rows(jnp.concatenate(fracs, axis=0))


def column_parts(column, offsets_ref, cell_z_ref):
    lanes = column_lanes(column)
    tile = iota((1, 256), 1) // 64
    from_x = iota((8, 256), 0) - offsets_ref[0:1, lanes]
    from_y = iota((16, 256), 0) - (offsets_ref[1:2, lanes] + 2 * tile)
    from_z = (iota((16, 256), 0) - cell_z_ref[:, lanes]) & 15
    return lanes, from_x, from_y, from_z


def blocks_z(owner_z, parts):
    zero = jnp.zeros((16, 256), BF16)
    return tuple(
        jnp.concatenate([jnp.where(owner_z == float(h), part, zero) for h in range(16)], axis=0)
        for part in parts
    )


def spread_kernel(
    counts_hbm, offsets_hbm, cell_z_hbm, frac_hbm, charges_hbm, table_hbm, out_ref, live_ref,
    slopes_ref, owner_ref, high_z_ref, low_z_ref, weight_x_ref, weight_y_ref, mesh_ref, packed_ref, counts_ref, offsets_ref, cell_z_ref, frac_ref, charges_ref, table_ref,
    sems,
):
    sources = [counts_hbm, offsets_hbm, cell_z_hbm, frac_hbm, charges_hbm, table_hbm]
    targets = [counts_ref, offsets_ref, cell_z_ref, frac_ref, charges_ref, table_ref]
    copies = [
        pltpu.make_async_copy(source, target, sems.at[i])
        for i, (source, target) in enumerate(zip(sources, targets))
    ]
    for copy in copies:
        copy.start()
    mesh_ref[...] = jnp.zeros_like(mesh_ref)
    for copy in copies:
        copy.wait()

    def pack(first, end):
        for x in range(first, end):
            packed_ref[PAD_Y * x : PAD_Y * (x + 1), :] = mesh_ref[16 * x : 16 * x + PAD_Y, :]

    def transform(first):
        section = split(packed_ref[first : first + 256, :])
        spectrum = dot3((table_ref[:K, :], table_ref[K:, :]), section, ((1,), (1,)))
        for j in range(2):
            out_ref[pl.ds(first // 128 + j, 256, stride=4), :] = spectrum[:, 128 * j : 128 * j + 128]

    values, slopes = group_splines(frac_ref)
    for j in range(6):
        slopes_ref[48 * j : 48 * j + 48, :] = slopes[j]
    for column in range(TILES_X):
        lanes, from_x, from_y, from_z = column_parts(column, offsets_ref, cell_z_ref)
        rows = [
            [value[3 * column + d : 3 * column + d + 1, :] for value in values] for d in range(3)
        ]
        owner_z = (((cell_z_ref[:, lanes] + from_z) & (K - 1)) >> 4).astype(F32).astype(BF16)
        lane = iota((1, 256), 1)
        counts = jnp.full((1, 256), counts_ref[4 * column], jnp.int32)
        for b in range(1, 4):
            counts = jnp.where(lane // 64 == b, counts_ref[4 * column + b], counts)
        live_q = jnp.where(lane % 64 < counts, charges_ref[:, lanes], 0.0)
        live_ref[:, lanes] = live_q
        weight_x = pick(from_x, rows[0]) * live_q
        weight_y = pick(from_y, rows[1])
        pair = jnp.concatenate([weight_x[i : i + 1, :] * weight_y for i in range(7)], axis=0)
        parts_z = split(pick(from_z, rows[2]))
        owner_ref[:, lanes] = owner_z
        high_z_ref[:, lanes], low_z_ref[:, lanes] = parts_z
        weight_x_ref[:, lanes] = weight_x
        weight_y_ref[:, lanes] = weight_y
        weight_z = blocks_z(owner_z, parts_z)
        place = slice(32 * column, 32 * column + 112)
        mesh_ref[place, :] += dot3(split(pair), weight_z, ((1,), (1,)))
        if column == 9:
            pack(0, 20)
            transform(0)

    packed_ref[USED:CHUNK, :] = jnp.zeros((CHUNK - USED, 256), F32)
    pack(20, PAD_X)
    transform(256)


def regroup(pieces, own, section):
    block = None
    for s, piece in enumerate(pieces):
        shift = (32 * (s - own)) % 128
        if shift:
            piece = pltpu.roll(piece, shift, 1)
        block = piece if block is None else jnp.where(section == s, piece, block)
    return block


def to_next(value, place):
    return jnp.where(place == 0, pltpu.roll(value, 97, 1), pltpu.roll(value, 1, 1))


def to_previous(value, place):
    return jnp.where(place == 31, pltpu.roll(value, 31, 1), pltpu.roll(value, 127, 1))


def plane_kernel(in_ref, plane_ref, order_ref, table_ref, out_ref, turned_ref, wide_ref):
    for j in range(4):
        turned = in_ref[pl.ds(j, 256, stride=4), :].T
        for h in range(2):
            turned_ref[h, 128 * j : 128 * j + 128, :] = turned[:, 128 * h : 128 * h + 128]
    turned_ref[:, CHUNK:, :] = jnp.zeros((2, SPARE, 128), F32)
    lane = iota((ROW_X, 128), 1)
    section = lane // 32
    place = lane % 32
    merged = []
    for h in range(2):
        lines = [turned_ref[h, pl.ds(y, ROW_X, stride=PAD_Y), :] for y in range(PAD_Y)]
        for y in range(PAD_Y - BLOCK_Y):
            lines[y] = lines[y] + to_next(lines[y + BLOCK_Y], place)
        merged.append(lines[:BLOCK_Y])
    beyond = iota((8, 128), 0) < PAD_X - BLOCK_X
    for quad in range(2):
        blocks = [
            regroup(merged[g // 4][4 * quad : 4 * quad + 4], g % 4, section) for g in range(N_GRP)
        ]
        for g in range(N_GRP):
            halo = jnp.where(beyond, blocks[g - 1][BLOCK_X:], 0.0)
            columns = slice(128 * quad, 128 * quad + 128)
            wide_ref[BLOCK_X * g : BLOCK_X * g + 8, columns] = blocks[g][:8] + halo
            wide_ref[BLOCK_X * g + 8 : BLOCK_X * (g + 1), columns] = blocks[g][8:BLOCK_X]
    order = (order_ref[:K, :], order_ref[K:, :])
    table = (table_ref[:K, :], table_ref[K:, :])
    half = dot3(split(wide_ref[...]), order)
    spectrum = dot3(table, split(half))
    mode = lax.axis_index("grp") * N_PEN + lax.axis_index("pen")
    lone = jnp.where(iota((2, 256), 1) == mode, plane_ref[2 * K :, :], 0.0)
    lone = jnp.sum(lone, axis=1, keepdims=True)
    square = plane_ref[K : 2 * K, :] + lone[1:2, :]
    nonzero = square > 0
    kernel = jnp.where(
        nonzero, plane_ref[:K, :] * lone[0:1, :] / jnp.where(nonzero, square, 1.0), 0.0
    )
    scaled = kernel * spectrum
    energy = jnp.sum(jnp.sum(scaled * spectrum, axis=0, keepdims=True), axis=1, keepdims=True)
    energy = energy * (0.5 / ATOMS)
    back = dot3(table, split(scaled))
    wide_ref[...] = dot3(split(back), order, ((1,), (1,)))
    for h in range(2):
        for quad in range(2):
            columns = slice(128 * quad, 128 * quad + 128)
            pieces = []
            for g in range(4 * h, 4 * h + 4):
                after = BLOCK_X * ((g + 1) % N_GRP)
                pieces.append(
                    jnp.concatenate(
                        [
                            wide_ref[BLOCK_X * g : BLOCK_X * (g + 1), columns],
                            wide_ref[after : after + 8, columns],
                        ],
                        axis=0,
                    )
                )
            for i in range(4):
                y = 4 * quad + i
                block = regroup(pieces, i, section)
                turned_ref[h, pl.ds(y, PAD_X, stride=PAD_Y), :] = block[:PAD_X]
                if y < PAD_Y - BLOCK_Y:
                    block = to_previous(block, place)
                    rows = pl.ds(y + BLOCK_Y, PAD_X, stride=PAD_Y)
                    turned_ref[h, rows, :] = block[:PAD_X]
        turned_ref[h, USED:CHUNK, :] = jnp.zeros((CHUNK - USED, 128), F32)
    spot = iota((256, 128), 1) == USED - 384
    for j in range(4):
        rows = slice(128 * j, 128 * j + 128)
        block = jnp.concatenate([turned_ref[0, rows, :], turned_ref[1, rows, :]], axis=1).T
        if j == 3:
            block = jnp.where(spot, energy, block)
        out_ref[pl.ds(j, 256, stride=4), :] = block


def force_kernel(
    offsets_ref, cell_z_ref, live_ref, slopes_ref, owner_ref, high_z_ref, low_z_ref, weight_x_ref,
    weight_y_ref, in_ref, table_ref, forces_ref, energy_ref,
    packed_ref, mesh_ref, mesh_high_ref, mesh_low_ref,
):
    table = (table_ref[:K, :], table_ref[K:, :])
    lane = iota((256, 128), 1)
    for j in range(4):
        chunk = in_ref[pl.ds(j, 256, stride=4), :]
        if j == 3:
            energies = jnp.where(lane == USED - 384, chunk, 0.0)
            energy_ref[...] = jnp.sum(
                jnp.sum(energies, axis=0, keepdims=True), axis=1, keepdims=True
            )
        packed_ref[128 * j : 128 * j + 128, :] = dot3(split(chunk.T), table)
    for x in range(PAD_X):
        mesh_ref[16 * x : 16 * x + 16, :] = packed_ref[PAD_Y * x : PAD_Y * x + 16, :]
    high, low = split(mesh_ref[...])
    mesh_high_ref[...] = high
    mesh_low_ref[...] = low

    for column in range(TILES_X):
        lanes, from_x, from_y, from_z = column_parts(column, offsets_ref, cell_z_ref)
        spots = [[48 * j + 3 * column + d for j in range(6)] for d in range(3)]
        grades = [[slopes_ref[spot : spot + 1, :] for spot in line] for line in spots]
        owner_z = owner_ref[:, lanes]
        weight_x = weight_x_ref[:, lanes]
        weight_y = weight_y_ref[:, lanes]
        live_q = live_ref[:, lanes]
        grade_x = pick(from_x, grades[0])
        grade_y = pick(from_y, grades[1])
        place = slice(32 * column, 32 * column + 112)
        footing = (mesh_high_ref[place, :], mesh_low_ref[place, :])
        main = dot3(footing, blocks_z(owner_z, (high_z_ref[:, lanes], low_z_ref[:, lanes])))
        tilt = dot3(footing, blocks_z(owner_z, split(pick(from_z, grades[2]))))
        sum_x = 0.0
        sum_y = 0.0
        sum_z = 0.0
        for i in range(7):
            band = main[16 * i : 16 * i + 16, :]
            sum_x = sum_x + grade_x[i : i + 1, :] * band
            sum_y = sum_y + weight_x[i : i + 1, :] * band
            sum_z = sum_z + weight_x[i : i + 1, :] * tilt[16 * i : 16 * i + 16, :]
        forces_ref[0:1, lanes] = -live_q * jnp.sum(weight_y * sum_x, axis=0, keepdims=True)
        forces_ref[1:2, lanes] = -jnp.sum(grade_y * sum_y, axis=0, keepdims=True)
        forces_ref[2:3, lanes] = -jnp.sum(weight_y * sum_z, axis=0, keepdims=True)


def call(kernel, out_shape, scratch, *args, memory=pltpu.VMEM):
    vmem = pl.BlockSpec(memory_space=pltpu.VMEM)
    return pl.pallas_call(
        kernel,
        out_shape=out_shape,
        in_specs=[pl.BlockSpec(memory_space=memory)] * len(args),
        out_specs=jax.tree.map(lambda _: vmem, out_shape),
        scratch_shapes=scratch,
        compiler_params=pltpu.CompilerParams(vmem_limit_bytes=8 * 1024 * 1024),
        cost_estimate=pl.CostEstimate(flops=3 * 10**9, bytes_accessed=10**7, transcendentals=0),
    )(*args)


def exchange(block):
    return lax.all_to_all(block.reshape(256, 4, 128), AXES, 0, 0, tiled=True).reshape(1024, 128)


def local(cell_offsets, cell_z, frac, charges, tile_counts):
    slots = charges.shape[0]
    cell_z = cell_z.reshape(1, slots)
    charges = charges.reshape(1, slots)
    table = jnp.asarray(TABLES["full"])
    block = jax.ShapeDtypeStruct((1024, 128), F32)
    sources = [tile_counts, cell_offsets, cell_z, frac, charges, table]
    outgoing, *kept = call(
        spread_kernel,
        (
            block,
            jax.ShapeDtypeStruct((1, slots), F32),
            jax.ShapeDtypeStruct((6 * 3 * TILES_X, 256), F32),
            jax.ShapeDtypeStruct((16, slots), BF16),
            jax.ShapeDtypeStruct((16, slots), BF16),
            jax.ShapeDtypeStruct((16, slots), BF16),
            jax.ShapeDtypeStruct((8, slots), F32),
            jax.ShapeDtypeStruct((16, slots), F32),
        ),
        [
            pltpu.VMEM((ROWS, 256), F32),
            pltpu.VMEM((CHUNK, 256), F32),
            pltpu.SMEM(tile_counts.shape, jnp.int32),
            *[pltpu.VMEM(source.shape, source.dtype) for source in sources[1:]],
            pltpu.SemaphoreType.DMA((len(sources),)),
        ],
        *[pltpu.with_memory_space_constraint(source, pltpu.HBM) for source in sources],
        memory=pltpu.HBM,
    )
    plane = exchange(outgoing)
    returning = call(
        plane_kernel,
        block,
        [pltpu.VMEM((2, CHUNK + SPARE, 128), F32), pltpu.VMEM((K, K), F32)],
        plane,
        jnp.asarray(TABLES["plane"]),
        jnp.asarray(TABLES["order"]),
        table,
    )
    home = exchange(returning)
    forces, energy = call(
        force_kernel,
        (jax.ShapeDtypeStruct((3, slots), F32), jax.ShapeDtypeStruct((1, 1), F32)),
        [
            pltpu.VMEM((CHUNK, 256), F32),
            pltpu.VMEM((ROWS, 256), F32),
            pltpu.VMEM((ROWS, 256), BF16),
            pltpu.VMEM((ROWS, 256), BF16),
        ],
        cell_offsets,
        cell_z,
        *kept,
        home,
        table,
    )
    return forces, energy.reshape(())


def solution(mesh):
    return jax.shard_map(
        local,
        mesh=mesh,
        in_specs=(P(None, AXES), P(AXES), P(None, AXES), P(AXES), P(AXES)),
        out_specs=(P(None, AXES), P()),
        check_vma=False,
    )
```

```python
import functools
import math

import jax
import jax.numpy as jnp
import numpy as np
from jax import lax
from jax.experimental import pallas as pl
from jax.experimental.pallas import tpu as pltpu
from jax.sharding import PartitionSpec as P

K = 256
ATOMS = 1048576
EWALD_SPLIT = 0.6
AXES = ("grp", "pen")
N_GRP = 8
N_PEN = 32
BLOCK_X = K // N_GRP
BLOCK_Y = K // N_PEN
TILES_X = BLOCK_X // 2
PAD_X = BLOCK_X + 5
PAD_Y = BLOCK_Y + 5
USED = PAD_X * PAD_Y
CHUNK = 512
ROWS = 16 * PAD_X
ROW_X = 40
SPARE = 16
F32 = jnp.float32
BF16 = jnp.bfloat16


def halves(table):
    high = table.astype(np.float32).astype(jnp.bfloat16)
    low = (table - high.astype(np.float64)).astype(np.float32).astype(jnp.bfloat16)
    return high, low


def cas(rows, columns):
    angle = (np.outer(rows, columns) % K) * (2.0 * math.pi / K)
    return np.cos(angle) + np.sin(angle)


def make_tables():
    index = np.arange(K)
    full = cas(index, index)
    order_y = (BLOCK_Y * np.arange(N_PEN)[None, :] + np.arange(BLOCK_Y)[:, None]).reshape(-1)
    frequency = np.where(2 * index < K, index, index - K) / K
    square = frequency * frequency
    coeffs = np.array([1.0, 26.0, 66.0, 26.0, 1.0]) / 120.0
    phase = np.exp(2j * math.pi * np.outer(index, np.arange(5)) / K)
    modulus = np.abs(phase @ coeffs) ** 2
    factor = np.exp(-(math.pi**2) * square / EWALD_SPLIT**2) / modulus
    plane_factor = np.outer(factor, factor) / (math.pi * float(K) ** 3)
    plane_square = square[:, None] + square[None, :]
    lone = np.stack([factor, square])
    return dict(
        full=np.concatenate(halves(full)),
        order=np.concatenate(halves(full[order_y])),
        plane=np.concatenate([plane_factor, plane_square, lone]).astype(np.float32),
    )


TABLES = make_tables()


def split(value):
    high = value.astype(BF16)
    low = (value - high.astype(F32)).astype(BF16)
    return high, low


def dot(left, right, dims=((1,), (0,))):
    return lax.dot_general(left, right, (dims, ((), ())), preferred_element_type=F32)


def dot3(left, right, dims=((1,), (0,))):
    size = left[0].shape[0]
    both = dot(jnp.concatenate(left, axis=0), right[0], dims)
    return both[:size] + both[size:] + dot(left[0], right[1], dims)


def spline_rows(fracs):
    values = [jnp.ones_like(fracs)]
    fifth = values
    for order in range(2, 7):
        scale = 1.0 / (order - 1)
        nxt = []
        for j in range(order):
            term = None
            if j >= 1:
                term = values[j - 1] * ((fracs + float(order - 1 - j)) * scale)
            if j <= order - 2:
                part = values[j] * ((float(1 + j) - fracs) * scale)
                term = part if term is None else term + part
            nxt.append(term)
        if order == 5:
            fifth = nxt
        values = nxt
    slopes = []
    for j in range(6):
        if j == 0:
            slopes.append(-fifth[0])
        elif j == 5:
            slopes.append(fifth[4])
        else:
            slopes.append(fifth[j - 1] - fifth[j])
    return values, slopes


def iota(shape, axis):
    return lax.broadcasted_iota(jnp.int32, shape, axis)


def pick(distance, rows):
    value = jnp.zeros(distance.shape, F32)
    for j in range(6):
        value = jnp.where(distance == j, rows[j], value)
    return value


def column_lanes(column):
    return slice(256 * column, 256 * column + 256)


def group_splines(frac_ref):
    fracs = [frac_ref[:, column_lanes(column)] for column in range(TILES_X)]
    return spline_rows(jnp.concatenate(fracs, axis=0))


def column_parts(column, offsets_ref, cell_z_ref):
    lanes = column_lanes(column)
    tile = iota((1, 256), 1) // 64
    from_x = iota((8, 256), 0) - offsets_ref[0:1, lanes]
    from_y = iota((16, 256), 0) - (offsets_ref[1:2, lanes] + 2 * tile)
    from_z = (iota((16, 256), 0) - cell_z_ref[:, lanes]) & 15
    return lanes, from_x, from_y, from_z


def blocks_z(owner_z, parts):
    zero = jnp.zeros((16, 256), BF16)
    return tuple(
        jnp.concatenate([jnp.where(owner_z == float(h), part, zero) for h in range(16)], axis=0)
        for part in parts
    )


def spread_kernel(
    counts_hbm, offsets_hbm, cell_z_hbm, frac_hbm, charges_hbm, table_hbm, out_ref, live_ref,
    slopes_ref, owner_ref, taps_z_ref, weight_x_ref, weight_y_ref, mesh_ref, packed_ref, counts_ref, offsets_ref, cell_z_ref, frac_ref, charges_ref, table_ref,
    sems,
):
    sources = [counts_hbm, offsets_hbm, cell_z_hbm, frac_hbm, charges_hbm, table_hbm]
    targets = [counts_ref, offsets_ref, cell_z_ref, frac_ref, charges_ref, table_ref]
    copies = [
        pltpu.make_async_copy(source, target, sems.at[i])
        for i, (source, target) in enumerate(zip(sources, targets))
    ]
    for copy in copies:
        copy.start()
    mesh_ref[...] = jnp.zeros_like(mesh_ref)
    for copy in copies:
        copy.wait()

    def pack(first, end):
        for x in range(first, end):
            packed_ref[PAD_Y * x : PAD_Y * (x + 1), :] = mesh_ref[16 * x : 16 * x + PAD_Y, :]

    def transform(first):
        section = split(packed_ref[first : first + 256, :])
        spectrum = dot3((table_ref[:K, :], table_ref[K:, :]), section, ((1,), (1,)))
        for j in range(2):
            out_ref[pl.ds(first // 128 + j, 256, stride=4), :] = spectrum[:, 128 * j : 128 * j + 128]

    values, slopes = group_splines(frac_ref)
    for j in range(6):
        slopes_ref[48 * j : 48 * j + 48, :] = slopes[j]
    for column in range(TILES_X):
        lanes, from_x, from_y, from_z = column_parts(column, offsets_ref, cell_z_ref)
        rows = [
            [value[3 * column + d : 3 * column + d + 1, :] for value in values] for d in range(3)
        ]
        owner_z = (((cell_z_ref[:, lanes] + from_z) & (K - 1)) >> 4).astype(F32)
        lane = iota((1, 256), 1)
        counts = jnp.full((1, 256), counts_ref[4 * column], jnp.int32)
        for b in range(1, 4):
            counts = jnp.where(lane // 64 == b, counts_ref[4 * column + b], counts)
        live_q = jnp.where(lane % 64 < counts, charges_ref[:, lanes], 0.0)
        live_ref[:, lanes] = live_q
        weight_x = pick(from_x, rows[0]) * live_q
        weight_y = pick(from_y, rows[1])
        pair = jnp.concatenate([weight_x[i : i + 1, :] * weight_y for i in range(7)], axis=0)
        taps_z = pick(from_z, rows[2])
        owner_ref[:, lanes] = owner_z
        taps_z_ref[:, lanes] = taps_z
        weight_x_ref[:, lanes] = weight_x
        weight_y_ref[:, lanes] = weight_y
        weight_z = blocks_z(owner_z.astype(BF16), split(taps_z))
        place = slice(32 * column, 32 * column + 112)
        mesh_ref[place, :] += dot3(split(pair), weight_z, ((1,), (1,)))
        if column == 9:
            pack(0, 20)
            transform(0)

    packed_ref[USED:CHUNK, :] = jnp.zeros((CHUNK - USED, 256), F32)
    pack(20, PAD_X)
    transform(256)


def regroup(pieces, own, section):
    block = None
    for s, piece in enumerate(pieces):
        shift = (32 * (s - own)) % 128
        if shift:
            piece = pltpu.roll(piece, shift, 1)
        block = piece if block is None else jnp.where(section == s, piece, block)
    return block


def to_next(value, place):
    return jnp.where(place == 0, pltpu.roll(value, 97, 1), pltpu.roll(value, 1, 1))


def to_previous(value, place):
    return jnp.where(place == 31, pltpu.roll(value, 31, 1), pltpu.roll(value, 127, 1))


def plane_kernel(in_ref, plane_ref, order_ref, table_ref, out_ref, turned_ref, wide_ref):
    for j in range(4):
        turned = in_ref[pl.ds(j, 256, stride=4), :].T
        for h in range(2):
            turned_ref[h, 128 * j : 128 * j + 128, :] = turned[:, 128 * h : 128 * h + 128]
    turned_ref[:, CHUNK:, :] = jnp.zeros((2, SPARE, 128), F32)
    lane = iota((ROW_X, 128), 1)
    section = lane // 32
    place = lane % 32
    merged = []
    for h in range(2):
        lines = [turned_ref[h, pl.ds(y, ROW_X, stride=PAD_Y), :] for y in range(PAD_Y)]
        for y in range(PAD_Y - BLOCK_Y):
            lines[y] = lines[y] + to_next(lines[y + BLOCK_Y], place)
        merged.append(lines[:BLOCK_Y])
    beyond = iota((8, 128), 0) < PAD_X - BLOCK_X
    for quad in range(2):
        blocks = [
            regroup(merged[g // 4][4 * quad : 4 * quad + 4], g % 4, section) for g in range(N_GRP)
        ]
        for g in range(N_GRP):
            halo = jnp.where(beyond, blocks[g - 1][BLOCK_X:], 0.0)
            columns = slice(128 * quad, 128 * quad + 128)
            wide_ref[BLOCK_X * g : BLOCK_X * g + 8, columns] = blocks[g][:8] + halo
            wide_ref[BLOCK_X * g + 8 : BLOCK_X * (g + 1), columns] = blocks[g][8:BLOCK_X]
    order = (order_ref[:K, :], order_ref[K:, :])
    table = (table_ref[:K, :], table_ref[K:, :])
    half = dot3(split(wide_ref[...]), order)
    spectrum = dot3(table, split(half))
    mode = lax.axis_index("grp") * N_PEN + lax.axis_index("pen")
    lone = jnp.where(iota((2, 256), 1) == mode, plane_ref[2 * K :, :], 0.0)
    lone = jnp.sum(lone, axis=1, keepdims=True)
    square = plane_ref[K : 2 * K, :] + lone[1:2, :]
    nonzero = square > 0
    kernel = jnp.where(
        nonzero, plane_ref[:K, :] * lone[0:1, :] / jnp.where(nonzero, square, 1.0), 0.0
    )
    scaled = kernel * spectrum
    energy = jnp.sum(jnp.sum(scaled * spectrum, axis=0, keepdims=True), axis=1, keepdims=True)
    energy = energy * (0.5 / ATOMS)
    back = dot3(table, split(scaled))
    wide_ref[...] = dot3(split(back), order, ((1,), (1,)))
    for h in range(2):
        for quad in range(2):
            columns = slice(128 * quad, 128 * quad + 128)
            pieces = []
            for g in range(4 * h, 4 * h + 4):
                after = BLOCK_X * ((g + 1) % N_GRP)
                pieces.append(
                    jnp.concatenate(
                        [
                            wide_ref[BLOCK_X * g : BLOCK_X * (g + 1), columns],
                            wide_ref[after : after + 8, columns],
                        ],
                        axis=0,
                    )
                )
            for i in range(4):
                y = 4 * quad + i
                block = regroup(pieces, i, section)
                turned_ref[h, pl.ds(y, PAD_X, stride=PAD_Y), :] = block[:PAD_X]
                if y < PAD_Y - BLOCK_Y:
                    block = to_previous(block, place)
                    rows = pl.ds(y + BLOCK_Y, PAD_X, stride=PAD_Y)
                    turned_ref[h, rows, :] = block[:PAD_X]
        turned_ref[h, USED:CHUNK, :] = jnp.zeros((CHUNK - USED, 128), F32)
    spot = iota((256, 128), 1) == USED - 384
    for j in range(4):
        rows = slice(128 * j, 128 * j + 128)
        block = jnp.concatenate([turned_ref[0, rows, :], turned_ref[1, rows, :]], axis=1).T
        if j == 3:
            block = jnp.where(spot, energy, block)
        out_ref[pl.ds(j, 256, stride=4), :] = block


def force_kernel(
    offsets_ref, cell_z_ref, live_ref, slopes_ref, owner_ref, taps_z_ref, weight_x_ref,
    weight_y_ref, in_ref, table_ref, forces_ref, energy_ref,
    packed_ref, mesh_ref, mesh_high_ref, mesh_low_ref,
):
    table = (table_ref[:K, :], table_ref[K:, :])
    lane = iota((256, 128), 1)
    for j in range(4):
        chunk = in_ref[pl.ds(j, 256, stride=4), :]
        if j == 3:
            energies = jnp.where(lane == USED - 384, chunk, 0.0)
            energy_ref[...] = jnp.sum(
                jnp.sum(energies, axis=0, keepdims=True), axis=1, keepdims=True
            )
        packed_ref[128 * j : 128 * j + 128, :] = dot3(split(chunk.T), table)
    for x in range(PAD_X):
        mesh_ref[16 * x : 16 * x + 16, :] = packed_ref[PAD_Y * x : PAD_Y * x + 16, :]
    high, low = split(mesh_ref[...])
    mesh_high_ref[...] = high
    mesh_low_ref[...] = low

    for column in range(TILES_X):
        lanes, from_x, from_y, from_z = column_parts(column, offsets_ref, cell_z_ref)
        spots = [[48 * j + 3 * column + d for j in range(6)] for d in range(3)]
        grades = [[slopes_ref[spot : spot + 1, :] for spot in line] for line in spots]
        owner_z = owner_ref[:, lanes].astype(BF16)
        weight_x = weight_x_ref[:, lanes]
        weight_y = weight_y_ref[:, lanes]
        live_q = live_ref[:, lanes]
        grade_x = pick(from_x, grades[0])
        grade_y = pick(from_y, grades[1])
        place = slice(32 * column, 32 * column + 112)
        footing = (mesh_high_ref[place, :], mesh_low_ref[place, :])
        main = dot3(footing, blocks_z(owner_z, split(taps_z_ref[:, lanes])))
        tilt = dot3(footing, blocks_z(owner_z, split(pick(from_z, grades[2]))))
        sum_x = 0.0
        sum_y = 0.0
        sum_z = 0.0
        for i in range(7):
            band = main[16 * i : 16 * i + 16, :]
            sum_x = sum_x + grade_x[i : i + 1, :] * band
            sum_y = sum_y + weight_x[i : i + 1, :] * band
            sum_z = sum_z + weight_x[i : i + 1, :] * tilt[16 * i : 16 * i + 16, :]
        forces_ref[0:1, lanes] = -live_q * jnp.sum(weight_y * sum_x, axis=0, keepdims=True)
        forces_ref[1:2, lanes] = -jnp.sum(grade_y * sum_y, axis=0, keepdims=True)
        forces_ref[2:3, lanes] = -jnp.sum(weight_y * sum_z, axis=0, keepdims=True)


def call(kernel, out_shape, scratch, *args, memory=pltpu.VMEM):
    vmem = pl.BlockSpec(memory_space=pltpu.VMEM)
    return pl.pallas_call(
        kernel,
        out_shape=out_shape,
        in_specs=[pl.BlockSpec(memory_space=memory)] * len(args),
        out_specs=jax.tree.map(lambda _: vmem, out_shape),
        scratch_shapes=scratch,
        compiler_params=pltpu.CompilerParams(vmem_limit_bytes=8 * 1024 * 1024),
        cost_estimate=pl.CostEstimate(flops=3 * 10**9, bytes_accessed=10**7, transcendentals=0),
    )(*args)


def exchange(block):
    return lax.all_to_all(block.reshape(256, 4, 128), AXES, 0, 0, tiled=True).reshape(1024, 128)


def local(cell_offsets, cell_z, frac, charges, tile_counts):
    slots = charges.shape[0]
    cell_z = cell_z.reshape(1, slots)
    charges = charges.reshape(1, slots)
    table = jnp.asarray(TABLES["full"])
    block = jax.ShapeDtypeStruct((1024, 128), F32)
    sources = [tile_counts, cell_offsets, cell_z, frac, charges, table]
    outgoing, *kept = call(
        spread_kernel,
        (
            block,
            jax.ShapeDtypeStruct((1, slots), F32),
            jax.ShapeDtypeStruct((6 * 3 * TILES_X, 256), F32),
            jax.ShapeDtypeStruct((16, slots), F32),
            jax.ShapeDtypeStruct((16, slots), F32),
            jax.ShapeDtypeStruct((8, slots), F32),
            jax.ShapeDtypeStruct((16, slots), F32),
        ),
        [
            pltpu.VMEM((ROWS, 256), F32),
            pltpu.VMEM((CHUNK, 256), F32),
            pltpu.SMEM(tile_counts.shape, jnp.int32),
            *[pltpu.VMEM(source.shape, source.dtype) for source in sources[1:]],
            pltpu.SemaphoreType.DMA((len(sources),)),
        ],
        *[pltpu.with_memory_space_constraint(source, pltpu.HBM) for source in sources],
        memory=pltpu.HBM,
    )
    plane = exchange(outgoing)
    returning = call(
        plane_kernel,
        block,
        [pltpu.VMEM((2, CHUNK + SPARE, 128), F32), pltpu.VMEM((K, K), F32)],
        plane,
        jnp.asarray(TABLES["plane"]),
        jnp.asarray(TABLES["order"]),
        table,
    )
    home = exchange(returning)
    forces, energy = call(
        force_kernel,
        (jax.ShapeDtypeStruct((3, slots), F32), jax.ShapeDtypeStruct((1, 1), F32)),
        [
            pltpu.VMEM((CHUNK, 256), F32),
            pltpu.VMEM((ROWS, 256), F32),
            pltpu.VMEM((ROWS, 256), BF16),
            pltpu.VMEM((ROWS, 256), BF16),
        ],
        cell_offsets,
        cell_z,
        *kept,
        home,
        table,
    )
    return forces, energy.reshape(())


def solution(mesh):
    return jax.shard_map(
        local,
        mesh=mesh,
        in_specs=(P(None, AXES), P(AXES), P(None, AXES), P(AXES), P(AXES)),
        out_specs=(P(None, AXES), P()),
        check_vma=False,
    )
```

```python
import functools
import math

import jax
import jax.numpy as jnp
import numpy as np
from jax import lax
from jax.experimental import pallas as pl
from jax.experimental.pallas import tpu as pltpu
from jax.sharding import PartitionSpec as P

K = 256
ATOMS = 1048576
EWALD_SPLIT = 0.6
AXES = ("grp", "pen")
N_GRP = 8
N_PEN = 32
BLOCK_X = K // N_GRP
BLOCK_Y = K // N_PEN
TILES_X = BLOCK_X // 2
PAD_X = BLOCK_X + 5
PAD_Y = BLOCK_Y + 5
USED = PAD_X * PAD_Y
CHUNK = 512
ROWS = 16 * PAD_X
ROW_X = 40
SPARE = 16
F32 = jnp.float32
BF16 = jnp.bfloat16


def halves(table):
    high = table.astype(np.float32).astype(jnp.bfloat16)
    low = (table - high.astype(np.float64)).astype(np.float32).astype(jnp.bfloat16)
    return high, low


def cas(rows, columns):
    angle = (np.outer(rows, columns) % K) * (2.0 * math.pi / K)
    return np.cos(angle) + np.sin(angle)


def make_tables():
    index = np.arange(K)
    full = cas(index, index)
    order_y = (BLOCK_Y * np.arange(N_PEN)[None, :] + np.arange(BLOCK_Y)[:, None]).reshape(-1)
    frequency = np.where(2 * index < K, index, index - K) / K
    square = frequency * frequency
    coeffs = np.array([1.0, 26.0, 66.0, 26.0, 1.0]) / 120.0
    phase = np.exp(2j * math.pi * np.outer(index, np.arange(5)) / K)
    modulus = np.abs(phase @ coeffs) ** 2
    factor = np.exp(-(math.pi**2) * square / EWALD_SPLIT**2) / modulus
    plane_factor = np.outer(factor, factor) / (math.pi * float(K) ** 3)
    plane_square = square[:, None] + square[None, :]
    lone = np.stack([factor, square])
    return dict(
        full=np.concatenate(halves(full)),
        order=np.concatenate(halves(full[order_y])),
        plane=np.concatenate([plane_factor, plane_square, lone]).astype(np.float32),
    )


TABLES = make_tables()


def split(value):
    high = value.astype(BF16)
    low = (value - high.astype(F32)).astype(BF16)
    return high, low


def dot(left, right, dims=((1,), (0,))):
    return lax.dot_general(left, right, (dims, ((), ())), preferred_element_type=F32)


def dot3(left, right, dims=((1,), (0,))):
    size = left[0].shape[0]
    both = dot(jnp.concatenate(left, axis=0), right[0], dims)
    return both[:size] + both[size:] + dot(left[0], right[1], dims)


def spline_rows(fracs):
    values = [jnp.ones_like(fracs)]
    fifth = values
    for order in range(2, 7):
        scale = 1.0 / (order - 1)
        nxt = []
        for j in range(order):
            term = None
            if j >= 1:
                term = values[j - 1] * ((fracs + float(order - 1 - j)) * scale)
            if j <= order - 2:
                part = values[j] * ((float(1 + j) - fracs) * scale)
                term = part if term is None else term + part
            nxt.append(term)
        if order == 5:
            fifth = nxt
        values = nxt
    slopes = []
    for j in range(6):
        if j == 0:
            slopes.append(-fifth[0])
        elif j == 5:
            slopes.append(fifth[4])
        else:
            slopes.append(fifth[j - 1] - fifth[j])
    return values, slopes


def iota(shape, axis):
    return lax.broadcasted_iota(jnp.int32, shape, axis)


def pick(distance, rows):
    value = jnp.zeros(distance.shape, F32)
    for j in range(6):
        value = jnp.where(distance == j, rows[j], value)
    return value


def column_lanes(column):
    return slice(256 * column, 256 * column + 256)


def group_splines(frac_ref):
    fracs = [frac_ref[:, column_lanes(column)] for column in range(TILES_X)]
    return spline_rows(jnp.concatenate(fracs, axis=0))


def column_parts(column, offsets_ref, cell_z_ref):
    lanes = column_lanes(column)
    tile = iota((1, 256), 1) // 64
    from_x = iota((8, 256), 0) - offsets_ref[0:1, lanes]
    from_y = iota((16, 256), 0) - (offsets_ref[1:2, lanes] + 2 * tile)
    from_z = (iota((16, 256), 0) - cell_z_ref[:, lanes]) & 15
    return lanes, from_x, from_y, from_z


def blocks_z(owner_z, parts):
    zero = jnp.zeros((16, 256), BF16)
    return tuple(
        jnp.concatenate([jnp.where(owner_z == float(h), part, zero) for h in range(16)], axis=0)
        for part in parts
    )


def spread_kernel(
    counts_hbm, offsets_hbm, cell_z_hbm, frac_hbm, charges_hbm, table_hbm, out_ref, live_ref,
    slopes_ref, owner_ref, taps_z_ref, weight_x_ref, weight_y_ref, mesh_ref, packed_ref, counts_ref, offsets_ref, cell_z_ref, frac_ref, charges_ref, table_ref,
    sems,
):
    sources = [frac_hbm, cell_z_hbm, offsets_hbm, charges_hbm, counts_hbm, table_hbm]
    targets = [frac_ref, cell_z_ref, offsets_ref, charges_ref, counts_ref, table_ref]
    copies = [
        pltpu.make_async_copy(source, target, sems.at[i])
        for i, (source, target) in enumerate(zip(sources, targets))
    ]
    for copy in copies:
        copy.start()
    mesh_ref[...] = jnp.zeros_like(mesh_ref)
    copies[0].wait()

    def pack(first, end):
        for x in range(first, end):
            packed_ref[PAD_Y * x : PAD_Y * (x + 1), :] = mesh_ref[16 * x : 16 * x + PAD_Y, :]

    def transform(first):
        section = split(packed_ref[first : first + 256, :])
        spectrum = dot3((table_ref[:K, :], table_ref[K:, :]), section, ((1,), (1,)))
        for j in range(2):
            out_ref[pl.ds(first // 128 + j, 256, stride=4), :] = spectrum[:, 128 * j : 128 * j + 128]

    values, slopes = group_splines(frac_ref)
    for j in range(6):
        slopes_ref[48 * j : 48 * j + 48, :] = slopes[j]
    for copy in copies[1:]:
        copy.wait()
    for column in range(TILES_X):
        lanes, from_x, from_y, from_z = column_parts(column, offsets_ref, cell_z_ref)
        rows = [
            [value[3 * column + d : 3 * column + d + 1, :] for value in values] for d in range(3)
        ]
        owner_z = (((cell_z_ref[:, lanes] + from_z) & (K - 1)) >> 4).astype(F32)
        lane = iota((1, 256), 1)
        counts = jnp.full((1, 256), counts_ref[4 * column], jnp.int32)
        for b in range(1, 4):
            counts = jnp.where(lane // 64 == b, counts_ref[4 * column + b], counts)
        live_q = jnp.where(lane % 64 < counts, charges_ref[:, lanes], 0.0)
        live_ref[:, lanes] = live_q
        weight_x = pick(from_x, rows[0]) * live_q
        weight_y = pick(from_y, rows[1])
        pair = jnp.concatenate([weight_x[i : i + 1, :] * weight_y for i in range(7)], axis=0)
        taps_z = pick(from_z, rows[2])
        owner_ref[:, lanes] = owner_z
        taps_z_ref[:, lanes] = taps_z
        weight_x_ref[:, lanes] = weight_x
        weight_y_ref[:, lanes] = weight_y
        weight_z = blocks_z(owner_z.astype(BF16), split(taps_z))
        place = slice(32 * column, 32 * column + 112)
        mesh_ref[place, :] += dot3(split(pair), weight_z, ((1,), (1,)))
        if column == 9:
            pack(0, 20)
            transform(0)

    packed_ref[USED:CHUNK, :] = jnp.zeros((CHUNK - USED, 256), F32)
    pack(20, PAD_X)
    transform(256)


def regroup(pieces, own, section):
    block = None
    for s, piece in enumerate(pieces):
        shift = (32 * (s - own)) % 128
        if shift:
            piece = pltpu.roll(piece, shift, 1)
        block = piece if block is None else jnp.where(section == s, piece, block)
    return block


def to_next(value, place):
    return jnp.where(place == 0, pltpu.roll(value, 97, 1), pltpu.roll(value, 1, 1))


def to_previous(value, place):
    return jnp.where(place == 31, pltpu.roll(value, 31, 1), pltpu.roll(value, 127, 1))


def plane_kernel(in_ref, plane_ref, order_ref, table_ref, out_ref, turned_ref, wide_ref):
    for j in range(4):
        turned = in_ref[pl.ds(j, 256, stride=4), :].T
        for h in range(2):
            turned_ref[h, 128 * j : 128 * j + 128, :] = turned[:, 128 * h : 128 * h + 128]
    turned_ref[:, CHUNK:, :] = jnp.zeros((2, SPARE, 128), F32)
    lane = iota((ROW_X, 128), 1)
    section = lane // 32
    place = lane % 32
    merged = []
    for h in range(2):
        lines = [turned_ref[h, pl.ds(y, ROW_X, stride=PAD_Y), :] for y in range(PAD_Y)]
        for y in range(PAD_Y - BLOCK_Y):
            lines[y] = lines[y] + to_next(lines[y + BLOCK_Y], place)
        merged.append(lines[:BLOCK_Y])
    beyond = iota((8, 128), 0) < PAD_X - BLOCK_X
    for quad in range(2):
        blocks = [
            regroup(merged[g // 4][4 * quad : 4 * quad + 4], g % 4, section) for g in range(N_GRP)
        ]
        for g in range(N_GRP):
            halo = jnp.where(beyond, blocks[g - 1][BLOCK_X:], 0.0)
            columns = slice(128 * quad, 128 * quad + 128)
            wide_ref[BLOCK_X * g : BLOCK_X * g + 8, columns] = blocks[g][:8] + halo
            wide_ref[BLOCK_X * g + 8 : BLOCK_X * (g + 1), columns] = blocks[g][8:BLOCK_X]
    order = (order_ref[:K, :], order_ref[K:, :])
    table = (table_ref[:K, :], table_ref[K:, :])
    half = dot3(split(wide_ref[...]), order)
    spectrum = dot3(table, split(half))
    mode = lax.axis_index("grp") * N_PEN + lax.axis_index("pen")
    lone = jnp.where(iota((2, 256), 1) == mode, plane_ref[2 * K :, :], 0.0)
    lone = jnp.sum(lone, axis=1, keepdims=True)
    square = plane_ref[K : 2 * K, :] + lone[1:2, :]
    nonzero = square > 0
    kernel = jnp.where(
        nonzero, plane_ref[:K, :] * lone[0:1, :] / jnp.where(nonzero, square, 1.0), 0.0
    )
    scaled = kernel * spectrum
    energy = jnp.sum(jnp.sum(scaled * spectrum, axis=0, keepdims=True), axis=1, keepdims=True)
    energy = energy * (0.5 / ATOMS)
    back = dot3(table, split(scaled))
    wide_ref[...] = dot3(split(back), order, ((1,), (1,)))
    for h in range(2):
        for quad in range(2):
            columns = slice(128 * quad, 128 * quad + 128)
            pieces = []
            for g in range(4 * h, 4 * h + 4):
                after = BLOCK_X * ((g + 1) % N_GRP)
                pieces.append(
                    jnp.concatenate(
                        [
                            wide_ref[BLOCK_X * g : BLOCK_X * (g + 1), columns],
                            wide_ref[after : after + 8, columns],
                        ],
                        axis=0,
                    )
                )
            for i in range(4):
                y = 4 * quad + i
                block = regroup(pieces, i, section)
                turned_ref[h, pl.ds(y, PAD_X, stride=PAD_Y), :] = block[:PAD_X]
                if y < PAD_Y - BLOCK_Y:
                    block = to_previous(block, place)
                    rows = pl.ds(y + BLOCK_Y, PAD_X, stride=PAD_Y)
                    turned_ref[h, rows, :] = block[:PAD_X]
        turned_ref[h, USED:CHUNK, :] = jnp.zeros((CHUNK - USED, 128), F32)
    spot = iota((256, 128), 1) == USED - 384
    for j in range(4):
        rows = slice(128 * j, 128 * j + 128)
        block = jnp.concatenate([turned_ref[0, rows, :], turned_ref[1, rows, :]], axis=1).T
        if j == 3:
            block = jnp.where(spot, energy, block)
        out_ref[pl.ds(j, 256, stride=4), :] = block


def force_kernel(
    offsets_ref, cell_z_ref, live_ref, slopes_ref, owner_ref, taps_z_ref, weight_x_ref,
    weight_y_ref, in_ref, table_ref, forces_ref, energy_ref,
    packed_ref, mesh_ref, mesh_high_ref, mesh_low_ref,
):
    table = (table_ref[:K, :], table_ref[K:, :])
    lane = iota((256, 128), 1)
    for j in range(4):
        chunk = in_ref[pl.ds(j, 256, stride=4), :]
        if j == 3:
            energies = jnp.where(lane == USED - 384, chunk, 0.0)
            energy_ref[...] = jnp.sum(
                jnp.sum(energies, axis=0, keepdims=True), axis=1, keepdims=True
            )
        packed_ref[128 * j : 128 * j + 128, :] = dot3(split(chunk.T), table)
    for x in range(PAD_X):
        mesh_ref[16 * x : 16 * x + 16, :] = packed_ref[PAD_Y * x : PAD_Y * x + 16, :]
    high, low = split(mesh_ref[...])
    mesh_high_ref[...] = high
    mesh_low_ref[...] = low

    for column in range(TILES_X):
        lanes, from_x, from_y, from_z = column_parts(column, offsets_ref, cell_z_ref)
        spots = [[48 * j + 3 * column + d for j in range(6)] for d in range(3)]
        grades = [[slopes_ref[spot : spot + 1, :] for spot in line] for line in spots]
        owner_z = owner_ref[:, lanes].astype(BF16)
        weight_x = weight_x_ref[:, lanes]
        weight_y = weight_y_ref[:, lanes]
        live_q = live_ref[:, lanes]
        grade_x = pick(from_x, grades[0])
        grade_y = pick(from_y, grades[1])
        place = slice(32 * column, 32 * column + 112)
        footing = (mesh_high_ref[place, :], mesh_low_ref[place, :])
        main = dot3(footing, blocks_z(owner_z, split(taps_z_ref[:, lanes])))
        tilt = dot3(footing, blocks_z(owner_z, split(pick(from_z, grades[2]))))
        sum_x = 0.0
        sum_y = 0.0
        sum_z = 0.0
        for i in range(7):
            band = main[16 * i : 16 * i + 16, :]
            sum_x = sum_x + grade_x[i : i + 1, :] * band
            sum_y = sum_y + weight_x[i : i + 1, :] * band
            sum_z = sum_z + weight_x[i : i + 1, :] * tilt[16 * i : 16 * i + 16, :]
        forces_ref[0:1, lanes] = -live_q * jnp.sum(weight_y * sum_x, axis=0, keepdims=True)
        forces_ref[1:2, lanes] = -jnp.sum(grade_y * sum_y, axis=0, keepdims=True)
        forces_ref[2:3, lanes] = -jnp.sum(weight_y * sum_z, axis=0, keepdims=True)


def call(kernel, out_shape, scratch, *args, memory=pltpu.VMEM):
    vmem = pl.BlockSpec(memory_space=pltpu.VMEM)
    return pl.pallas_call(
        kernel,
        out_shape=out_shape,
        in_specs=[pl.BlockSpec(memory_space=memory)] * len(args),
        out_specs=jax.tree.map(lambda _: vmem, out_shape),
        scratch_shapes=scratch,
        compiler_params=pltpu.CompilerParams(vmem_limit_bytes=8 * 1024 * 1024),
        cost_estimate=pl.CostEstimate(flops=3 * 10**9, bytes_accessed=10**7, transcendentals=0),
    )(*args)


def exchange(block):
    return lax.all_to_all(block.reshape(256, 4, 128), AXES, 0, 0, tiled=True).reshape(1024, 128)


def local(cell_offsets, cell_z, frac, charges, tile_counts):
    slots = charges.shape[0]
    cell_z = cell_z.reshape(1, slots)
    charges = charges.reshape(1, slots)
    table = jnp.asarray(TABLES["full"])
    block = jax.ShapeDtypeStruct((1024, 128), F32)
    sources = [tile_counts, cell_offsets, cell_z, frac, charges, table]
    outgoing, *kept = call(
        spread_kernel,
        (
            block,
            jax.ShapeDtypeStruct((1, slots), F32),
            jax.ShapeDtypeStruct((6 * 3 * TILES_X, 256), F32),
            jax.ShapeDtypeStruct((16, slots), F32),
            jax.ShapeDtypeStruct((16, slots), F32),
            jax.ShapeDtypeStruct((8, slots), F32),
            jax.ShapeDtypeStruct((16, slots), F32),
        ),
        [
            pltpu.VMEM((ROWS, 256), F32),
            pltpu.VMEM((CHUNK, 256), F32),
            pltpu.SMEM(tile_counts.shape, jnp.int32),
            *[pltpu.VMEM(source.shape, source.dtype) for source in sources[1:]],
            pltpu.SemaphoreType.DMA((len(sources),)),
        ],
        *[pltpu.with_memory_space_constraint(source, pltpu.HBM) for source in sources],
        memory=pltpu.HBM,
    )
    plane = exchange(outgoing)
    returning = call(
        plane_kernel,
        block,
        [pltpu.VMEM((2, CHUNK + SPARE, 128), F32), pltpu.VMEM((K, K), F32)],
        plane,
        jnp.asarray(TABLES["plane"]),
        jnp.asarray(TABLES["order"]),
        table,
    )
    home = exchange(returning)
    forces, energy = call(
        force_kernel,
        (jax.ShapeDtypeStruct((3, slots), F32), jax.ShapeDtypeStruct((1, 1), F32)),
        [
            pltpu.VMEM((CHUNK, 256), F32),
            pltpu.VMEM((ROWS, 256), F32),
            pltpu.VMEM((ROWS, 256), BF16),
            pltpu.VMEM((ROWS, 256), BF16),
        ],
        cell_offsets,
        cell_z,
        *kept,
        home,
        table,
    )
    return forces, energy.reshape(())


def solution(mesh):
    return jax.shard_map(
        local,
        mesh=mesh,
        in_specs=(P(None, AXES), P(AXES), P(None, AXES), P(AXES), P(AXES)),
        out_specs=(P(None, AXES), P()),
        check_vma=False,
    )
```

```python
import functools
import math

import jax
import jax.numpy as jnp
import numpy as np
from jax import lax
from jax.experimental import pallas as pl
from jax.experimental.pallas import tpu as pltpu
from jax.sharding import PartitionSpec as P

K = 256
ATOMS = 1048576
EWALD_SPLIT = 0.6
AXES = ("grp", "pen")
N_GRP = 8
N_PEN = 32
BLOCK_X = K // N_GRP
BLOCK_Y = K // N_PEN
TILES_X = BLOCK_X // 2
PAD_X = BLOCK_X + 5
PAD_Y = BLOCK_Y + 5
USED = PAD_X * PAD_Y
CHUNK = 512
ROWS = 16 * PAD_X
ROW_X = 40
SPARE = 16
F32 = jnp.float32
BF16 = jnp.bfloat16


def halves(table):
    high = table.astype(np.float32).astype(jnp.bfloat16)
    low = (table - high.astype(np.float64)).astype(np.float32).astype(jnp.bfloat16)
    return high, low


def cas(rows, columns):
    angle = (np.outer(rows, columns) % K) * (2.0 * math.pi / K)
    return np.cos(angle) + np.sin(angle)


def make_tables():
    index = np.arange(K)
    full = cas(index, index)
    order_y = (BLOCK_Y * np.arange(N_PEN)[None, :] + np.arange(BLOCK_Y)[:, None]).reshape(-1)
    frequency = np.where(2 * index < K, index, index - K) / K
    square = frequency * frequency
    coeffs = np.array([1.0, 26.0, 66.0, 26.0, 1.0]) / 120.0
    phase = np.exp(2j * math.pi * np.outer(index, np.arange(5)) / K)
    modulus = np.abs(phase @ coeffs) ** 2
    factor = np.exp(-(math.pi**2) * square / EWALD_SPLIT**2) / modulus
    plane_factor = np.outer(factor, factor) / (math.pi * float(K) ** 3)
    plane_square = square[:, None] + square[None, :]
    lone = np.stack([factor, square])
    return dict(
        full=np.concatenate(halves(full)),
        order=np.concatenate(halves(full[order_y])),
        plane=np.concatenate([plane_factor, plane_square, lone]).astype(np.float32),
    )


TABLES = make_tables()


def split(value):
    high = value.astype(BF16)
    low = (value - high.astype(F32)).astype(BF16)
    return high, low


def dot(left, right, dims=((1,), (0,))):
    return lax.dot_general(left, right, (dims, ((), ())), preferred_element_type=F32)


def dot3(left, right, dims=((1,), (0,))):
    size = left[0].shape[0]
    both = dot(jnp.concatenate(left, axis=0), right[0], dims)
    return both[:size] + both[size:] + dot(left[0], right[1], dims)


def spline_rows(fracs):
    values = [jnp.ones_like(fracs)]
    fifth = values
    for order in range(2, 7):
        scale = 1.0 / (order - 1)
        nxt = []
        for j in range(order):
            term = None
            if j >= 1:
                term = values[j - 1] * ((fracs + float(order - 1 - j)) * scale)
            if j <= order - 2:
                part = values[j] * ((float(1 + j) - fracs) * scale)
                term = part if term is None else term + part
            nxt.append(term)
        if order == 5:
            fifth = nxt
        values = nxt
    slopes = []
    for j in range(6):
        if j == 0:
            slopes.append(-fifth[0])
        elif j == 5:
            slopes.append(fifth[4])
        else:
            slopes.append(fifth[j - 1] - fifth[j])
    return values, slopes


def iota(shape, axis):
    return lax.broadcasted_iota(jnp.int32, shape, axis)


def pick(distance, rows):
    value = jnp.zeros(distance.shape, F32)
    for j in range(6):
        value = jnp.where(distance == j, rows[j], value)
    return value


def column_lanes(column):
    return slice(256 * column, 256 * column + 256)


def group_splines(frac_ref):
    fracs = [frac_ref[:, column_lanes(column)] for column in range(TILES_X)]
    return spline_rows(jnp.concatenate(fracs, axis=0))


def column_parts(column, offsets_ref, cell_z_ref):
    lanes = column_lanes(column)
    tile = iota((1, 256), 1) // 64
    from_x = iota((8, 256), 0) - offsets_ref[0:1, lanes]
    from_y = iota((16, 256), 0) - (offsets_ref[1:2, lanes] + 2 * tile)
    from_z = (iota((16, 256), 0) - cell_z_ref[:, lanes]) & 15
    return lanes, from_x, from_y, from_z


def blocks_z(owner_z, parts):
    zero = jnp.zeros((16, 256), BF16)
    return tuple(
        jnp.concatenate([jnp.where(owner_z == float(h), part, zero) for h in range(16)], axis=0)
        for part in parts
    )


def spread_kernel(
    counts_hbm, offsets_hbm, cell_z_hbm, frac_hbm, charges_hbm, table_hbm, out_ref, live_ref,
    slopes_ref, owner_ref, taps_z_ref, weight_x_ref, weight_y_ref, mesh_ref, packed_ref, counts_ref, offsets_ref, cell_z_ref, frac_ref, charges_ref, table_ref,
    sems,
):
    sources = [frac_hbm, cell_z_hbm, offsets_hbm, charges_hbm, counts_hbm, table_hbm]
    targets = [frac_ref, cell_z_ref, offsets_ref, charges_ref, counts_ref, table_ref]
    copies = [
        pltpu.make_async_copy(source, target, sems.at[i])
        for i, (source, target) in enumerate(zip(sources, targets))
    ]
    for copy in copies:
        copy.start()
    copies[0].wait()

    def pack(first, end):
        for x in range(first, end):
            packed_ref[PAD_Y * x : PAD_Y * (x + 1), :] = mesh_ref[16 * x : 16 * x + PAD_Y, :]

    def transform(first):
        section = split(packed_ref[first : first + 256, :])
        spectrum = dot3((table_ref[:K, :], table_ref[K:, :]), section, ((1,), (1,)))
        for j in range(2):
            out_ref[pl.ds(first // 128 + j, 256, stride=4), :] = spectrum[:, 128 * j : 128 * j + 128]

    values, slopes = group_splines(frac_ref)
    for j in range(6):
        slopes_ref[48 * j : 48 * j + 48, :] = slopes[j]
    for copy in copies[1:]:
        copy.wait()
    for column in range(TILES_X):
        lanes, from_x, from_y, from_z = column_parts(column, offsets_ref, cell_z_ref)
        rows = [
            [value[3 * column + d : 3 * column + d + 1, :] for value in values] for d in range(3)
        ]
        owner_z = (((cell_z_ref[:, lanes] + from_z) & (K - 1)) >> 4).astype(F32)
        lane = iota((1, 256), 1)
        counts = jnp.full((1, 256), counts_ref[4 * column], jnp.int32)
        for b in range(1, 4):
            counts = jnp.where(lane // 64 == b, counts_ref[4 * column + b], counts)
        live_q = jnp.where(lane % 64 < counts, charges_ref[:, lanes], 0.0)
        live_ref[:, lanes] = live_q
        weight_x = pick(from_x, rows[0]) * live_q
        weight_y = pick(from_y, rows[1])
        pair = jnp.concatenate([weight_x[i : i + 1, :] * weight_y for i in range(7)], axis=0)
        taps_z = pick(from_z, rows[2])
        owner_ref[:, lanes] = owner_z
        taps_z_ref[:, lanes] = taps_z
        weight_x_ref[:, lanes] = weight_x
        weight_y_ref[:, lanes] = weight_y
        weight_z = blocks_z(owner_z.astype(BF16), split(taps_z))
        part = dot3(split(pair), weight_z, ((1,), (1,)))
        top = 32 * column
        fresh = top + 80 if column else 0
        if column:
            mesh_ref[top:fresh, :] += part[:80, :]
        mesh_ref[fresh : top + 112, :] = part[fresh - top :, :]
        if column == 9:
            pack(0, 20)
            transform(0)

    packed_ref[USED:CHUNK, :] = jnp.zeros((CHUNK - USED, 256), F32)
    pack(20, PAD_X)
    transform(256)


def regroup(pieces, own, section):
    block = None
    for s, piece in enumerate(pieces):
        shift = (32 * (s - own)) % 128
        if shift:
            piece = pltpu.roll(piece, shift, 1)
        block = piece if block is None else jnp.where(section == s, piece, block)
    return block


def to_next(value, place):
    return jnp.where(place == 0, pltpu.roll(value, 97, 1), pltpu.roll(value, 1, 1))


def to_previous(value, place):
    return jnp.where(place == 31, pltpu.roll(value, 31, 1), pltpu.roll(value, 127, 1))


def plane_kernel(in_ref, plane_ref, order_ref, table_ref, out_ref, turned_ref, wide_ref):
    for j in range(4):
        turned = in_ref[pl.ds(j, 256, stride=4), :].T
        for h in range(2):
            turned_ref[h, 128 * j : 128 * j + 128, :] = turned[:, 128 * h : 128 * h + 128]
    turned_ref[:, CHUNK:, :] = jnp.zeros((2, SPARE, 128), F32)
    lane = iota((ROW_X, 128), 1)
    section = lane // 32
    place = lane % 32
    merged = []
    for h in range(2):
        lines = [turned_ref[h, pl.ds(y, ROW_X, stride=PAD_Y), :] for y in range(PAD_Y)]
        for y in range(PAD_Y - BLOCK_Y):
            lines[y] = lines[y] + to_next(lines[y + BLOCK_Y], place)
        merged.append(lines[:BLOCK_Y])
    beyond = iota((8, 128), 0) < PAD_X - BLOCK_X
    for quad in range(2):
        blocks = [
            regroup(merged[g // 4][4 * quad : 4 * quad + 4], g % 4, section) for g in range(N_GRP)
        ]
        for g in range(N_GRP):
            halo = jnp.where(beyond, blocks[g - 1][BLOCK_X:], 0.0)
            columns = slice(128 * quad, 128 * quad + 128)
            wide_ref[BLOCK_X * g : BLOCK_X * g + 8, columns] = blocks[g][:8] + halo
            wide_ref[BLOCK_X * g + 8 : BLOCK_X * (g + 1), columns] = blocks[g][8:BLOCK_X]
    order = (order_ref[:K, :], order_ref[K:, :])
    table = (table_ref[:K, :], table_ref[K:, :])
    half = dot3(split(wide_ref[...]), order)
    spectrum = dot3(table, split(half))
    mode = lax.axis_index("grp") * N_PEN + lax.axis_index("pen")
    lone = jnp.where(iota((2, 256), 1) == mode, plane_ref[2 * K :, :], 0.0)
    lone = jnp.sum(lone, axis=1, keepdims=True)
    square = plane_ref[K : 2 * K, :] + lone[1:2, :]
    nonzero = square > 0
    kernel = jnp.where(
        nonzero, plane_ref[:K, :] * lone[0:1, :] / jnp.where(nonzero, square, 1.0), 0.0
    )
    scaled = kernel * spectrum
    energy = jnp.sum(jnp.sum(scaled * spectrum, axis=0, keepdims=True), axis=1, keepdims=True)
    energy = energy * (0.5 / ATOMS)
    back = dot3(table, split(scaled))
    wide_ref[...] = dot3(split(back), order, ((1,), (1,)))
    for h in range(2):
        for quad in range(2):
            columns = slice(128 * quad, 128 * quad + 128)
            pieces = []
            for g in range(4 * h, 4 * h + 4):
                after = BLOCK_X * ((g + 1) % N_GRP)
                pieces.append(
                    jnp.concatenate(
                        [
                            wide_ref[BLOCK_X * g : BLOCK_X * (g + 1), columns],
                            wide_ref[after : after + 8, columns],
                        ],
                        axis=0,
                    )
                )
            for i in range(4):
                y = 4 * quad + i
                block = regroup(pieces, i, section)
                turned_ref[h, pl.ds(y, PAD_X, stride=PAD_Y), :] = block[:PAD_X]
                if y < PAD_Y - BLOCK_Y:
                    block = to_previous(block, place)
                    rows = pl.ds(y + BLOCK_Y, PAD_X, stride=PAD_Y)
                    turned_ref[h, rows, :] = block[:PAD_X]
        turned_ref[h, USED:CHUNK, :] = jnp.zeros((CHUNK - USED, 128), F32)
    spot = iota((256, 128), 1) == USED - 384
    for j in range(4):
        rows = slice(128 * j, 128 * j + 128)
        block = jnp.concatenate([turned_ref[0, rows, :], turned_ref[1, rows, :]], axis=1).T
        if j == 3:
            block = jnp.where(spot, energy, block)
        out_ref[pl.ds(j, 256, stride=4), :] = block


def force_kernel(
    offsets_ref, cell_z_ref, live_ref, slopes_ref, owner_ref, taps_z_ref, weight_x_ref,
    weight_y_ref, in_ref, table_ref, forces_ref, energy_ref,
    packed_ref, mesh_ref, mesh_high_ref, mesh_low_ref,
):
    table = (table_ref[:K, :], table_ref[K:, :])
    lane = iota((256, 128), 1)
    for j in range(4):
        chunk = in_ref[pl.ds(j, 256, stride=4), :]
        if j == 3:
            energies = jnp.where(lane == USED - 384, chunk, 0.0)
            energy_ref[...] = jnp.sum(
                jnp.sum(energies, axis=0, keepdims=True), axis=1, keepdims=True
            )
        packed_ref[128 * j : 128 * j + 128, :] = dot3(split(chunk.T), table)
    for x in range(PAD_X):
        mesh_ref[16 * x : 16 * x + 16, :] = packed_ref[PAD_Y * x : PAD_Y * x + 16, :]
    high, low = split(mesh_ref[...])
    mesh_high_ref[...] = high
    mesh_low_ref[...] = low

    for column in range(TILES_X):
        lanes, from_x, from_y, from_z = column_parts(column, offsets_ref, cell_z_ref)
        spots = [[48 * j + 3 * column + d for j in range(6)] for d in range(3)]
        grades = [[slopes_ref[spot : spot + 1, :] for spot in line] for line in spots]
        owner_z = owner_ref[:, lanes].astype(BF16)
        weight_x = weight_x_ref[:, lanes]
        weight_y = weight_y_ref[:, lanes]
        live_q = live_ref[:, lanes]
        grade_x = pick(from_x, grades[0])
        grade_y = pick(from_y, grades[1])
        place = slice(32 * column, 32 * column + 112)
        footing = (mesh_high_ref[place, :], mesh_low_ref[place, :])
        main = dot3(footing, blocks_z(owner_z, split(taps_z_ref[:, lanes])))
        tilt = dot3(footing, blocks_z(owner_z, split(pick(from_z, grades[2]))))
        sum_x = 0.0
        sum_y = 0.0
        sum_z = 0.0
        for i in range(7):
            band = main[16 * i : 16 * i + 16, :]
            sum_x = sum_x + grade_x[i : i + 1, :] * band
            sum_y = sum_y + weight_x[i : i + 1, :] * band
            sum_z = sum_z + weight_x[i : i + 1, :] * tilt[16 * i : 16 * i + 16, :]
        forces_ref[0:1, lanes] = -live_q * jnp.sum(weight_y * sum_x, axis=0, keepdims=True)
        forces_ref[1:2, lanes] = -jnp.sum(grade_y * sum_y, axis=0, keepdims=True)
        forces_ref[2:3, lanes] = -jnp.sum(weight_y * sum_z, axis=0, keepdims=True)


def call(kernel, out_shape, scratch, *args, memory=pltpu.VMEM):
    vmem = pl.BlockSpec(memory_space=pltpu.VMEM)
    return pl.pallas_call(
        kernel,
        out_shape=out_shape,
        in_specs=[pl.BlockSpec(memory_space=memory)] * len(args),
        out_specs=jax.tree.map(lambda _: vmem, out_shape),
        scratch_shapes=scratch,
        compiler_params=pltpu.CompilerParams(vmem_limit_bytes=8 * 1024 * 1024),
        cost_estimate=pl.CostEstimate(flops=3 * 10**9, bytes_accessed=10**7, transcendentals=0),
    )(*args)


def exchange(block):
    return lax.all_to_all(block.reshape(256, 4, 128), AXES, 0, 0, tiled=True).reshape(1024, 128)


def local(cell_offsets, cell_z, frac, charges, tile_counts):
    slots = charges.shape[0]
    cell_z = cell_z.reshape(1, slots)
    charges = charges.reshape(1, slots)
    table = jnp.asarray(TABLES["full"])
    block = jax.ShapeDtypeStruct((1024, 128), F32)
    sources = [tile_counts, cell_offsets, cell_z, frac, charges, table]
    outgoing, *kept = call(
        spread_kernel,
        (
            block,
            jax.ShapeDtypeStruct((1, slots), F32),
            jax.ShapeDtypeStruct((6 * 3 * TILES_X, 256), F32),
            jax.ShapeDtypeStruct((16, slots), F32),
            jax.ShapeDtypeStruct((16, slots), F32),
            jax.ShapeDtypeStruct((8, slots), F32),
            jax.ShapeDtypeStruct((16, slots), F32),
        ),
        [
            pltpu.VMEM((ROWS, 256), F32),
            pltpu.VMEM((CHUNK, 256), F32),
            pltpu.SMEM(tile_counts.shape, jnp.int32),
            *[pltpu.VMEM(source.shape, source.dtype) for source in sources[1:]],
            pltpu.SemaphoreType.DMA((len(sources),)),
        ],
        *[pltpu.with_memory_space_constraint(source, pltpu.HBM) for source in sources],
        memory=pltpu.HBM,
    )
    plane = exchange(outgoing)
    returning = call(
        plane_kernel,
        block,
        [pltpu.VMEM((2, CHUNK + SPARE, 128), F32), pltpu.VMEM((K, K), F32)],
        plane,
        jnp.asarray(TABLES["plane"]),
        jnp.asarray(TABLES["order"]),
        table,
    )
    home = exchange(returning)
    forces, energy = call(
        force_kernel,
        (jax.ShapeDtypeStruct((3, slots), F32), jax.ShapeDtypeStruct((1, 1), F32)),
        [
            pltpu.VMEM((CHUNK, 256), F32),
            pltpu.VMEM((ROWS, 256), F32),
            pltpu.VMEM((ROWS, 256), BF16),
            pltpu.VMEM((ROWS, 256), BF16),
        ],
        cell_offsets,
        cell_z,
        *kept,
        home,
        table,
    )
    return forces, energy.reshape(())


def solution(mesh):
    return jax.shard_map(
        local,
        mesh=mesh,
        in_specs=(P(None, AXES), P(AXES), P(None, AXES), P(AXES), P(AXES)),
        out_specs=(P(None, AXES), P()),
        check_vma=False,
    )
```
